128 devices in a mesh: batch: 1, col: 2 (over core), row: 64 (over z, y, x).
Axes of the slice: x: 4, y: 4, z: 4, core: 2. Of those that a mesh axis runs over, the one named last changes fastest.
Arguments:
- x: bfloat16 [16, 512, 128, 256], P('batch', 'row', 'col')
- w_down_1: bfloat16 [3, 3, 256, 512], replicated
- b_down_1: float32 [512], replicated
- w_conv_1: bfloat16 [3, 3, 512, 512], replicated
- b_conv_1: float32 [512], replicated
- w_proj_1: bfloat16 [256, 512], replicated
- w_down_2: bfloat16 [3, 3, 512, 1024], replicated
- b_down_2: float32 [1024], replicated
- w_conv_2: bfloat16 [3, 3, 1024, 1024], replicated
- b_conv_2: float32 [1024], replicated
- w_proj_2: bfloat16 [512, 1024], replicated
- w_down_3: bfloat16 [3, 3, 1024, 2048], replicated
- b_down_3: float32 [2048], replicated
- w_conv_3: bfloat16 [3, 3, 2048, 2048], replicated
- b_conv_3: float32 [2048], replicated
- w_proj_3: bfloat16 [1024, 2048], replicated
Outputs:
- output: bfloat16 [16, 64, 16, 2048], P('batch', 'row', 'col')
All inputs are finite; a program needn't handle non-finite values.
Results may differ from the reference program's by a relative error of at most 0.00593535.
Values are sent between devices in bfloat16 or wider.
A program may use at most 1 GiB of HBM per device.

```python
import jax
import jax.numpy as jnp
from jax import lax

IMAGES = 16
TILE_H = 8
TILE_W = 64
ROW_DEVS = 64
COL_DEVS = 2
CHAN_0 = 256
CHAN_1 = 512
CHAN_2 = 1024
CHAN_3 = 2048
HEIGHT = TILE_H * ROW_DEVS
WIDTH = TILE_W * COL_DEVS
CONV_DIMS = ("NHWC", "HWIO", "NHWC")


def setup_inputs(seed: int = 0, part: int = 0) -> dict:
    root_key = jax.random.key(seed)
    image_key = jax.random.fold_in(jax.random.fold_in(root_key, 1), part)
    inputs = {"x": jax.random.normal(image_key, (IMAGES, HEIGHT, WIDTH, CHAN_0), jnp.float32).astype(jnp.bfloat16)}
    widths = (CHAN_0, CHAN_1, CHAN_2, CHAN_3)
    for stage in range(3):
        c_in = widths[stage]
        c_out = widths[stage + 1]
        stage_keys = jax.random.split(jax.random.fold_in(root_key, 10 + stage), 5)
        suffix = str(stage + 1)
        inputs["w_down_" + suffix] = (jax.random.normal(stage_keys[0], (3, 3, c_in, c_out), jnp.float32) * (9 * c_in) ** -0.5).astype(jnp.bfloat16)
        inputs["b_down_" + suffix] = 0.5 * jax.random.normal(stage_keys[1], (c_out,), jnp.float32)
        inputs["w_conv_" + suffix] = (jax.random.normal(stage_keys[2], (3, 3, c_out, c_out), jnp.float32) * (9 * c_out) ** -0.5).astype(jnp.bfloat16)
        inputs["b_conv_" + suffix] = 0.5 * jax.random.normal(stage_keys[3], (c_out,), jnp.float32)
        inputs["w_proj_" + suffix] = (jax.random.normal(stage_keys[4], (c_in, c_out), jnp.float32) * c_in ** -0.5).astype(jnp.bfloat16)
    return inputs


def conv_same(act_in, weight, stride):
    return lax.conv_general_dilated(act_in.astype(jnp.float32), weight.astype(jnp.float32), (stride, stride), ((1, 1), (1, 1)), dimension_numbers=CONV_DIMS)


def basic_block(z_prev, w_down, b_down, w_conv, b_conv, w_proj):
    y_act = jax.nn.relu(conv_same(z_prev, w_down, 2) + b_down).astype(jnp.bfloat16)
    shortcut = jnp.einsum("bhwc,cd->bhwd", z_prev[:, ::2, ::2].astype(jnp.float32), w_proj.astype(jnp.float32))
    return jax.nn.relu(conv_same(y_act, w_conv, 1) + shortcut + b_conv).astype(jnp.bfloat16)


def reference(x, w_down_1, b_down_1, w_conv_1, b_conv_1, w_proj_1, w_down_2, b_down_2, w_conv_2, b_conv_2, w_proj_2, w_down_3, b_down_3, w_conv_3, b_conv_3, w_proj_3):
    params = ((w_down_1, b_down_1, w_conv_1, b_conv_1, w_proj_1), (w_down_2, b_down_2, w_conv_2, b_conv_2, w_proj_2), (w_down_3, b_down_3, w_conv_3, b_conv_3, w_proj_3))

    def one_image(image):
        act_out = image[None]
        for stage_params in params:
            act_out = basic_block(act_out, stage_params[0], stage_params[1], stage_params[2], stage_params[3], stage_params[4])
        return act_out[0]

    return lax.map(one_image, x)
```

```python
import jax
import jax.numpy as jnp
from jax import lax
from jax.experimental import pallas as pl
from jax.experimental.pallas import tpu as pltpu
from jax.sharding import PartitionSpec as P

F32 = jnp.float32
BF16 = jnp.bfloat16
RING = 8
GROUPS = (
    [("down", 2, kx, 0) for kx in range(3)]
    + [("down", 1, kx, 0) for kx in range(3)]
    + [("proj", 0, 0, 0)]
    + [("down", 0, kx, 0) for kx in range(3)]
    + [("conv", ky, kx, kh) for ky in (1, 0, 2) for kx in range(3) for kh in range(2)]
)
CONV_0 = 10


def encoder_kernel(rows, cols, x_ref, wd1, wc1, wp1, wd2, wc2, wp2, wd3, wc3, wp3, bd1, bc1, bd2, bc2, bd3, bc3, out_ref,
                   xp, y1p, z1p, y2p, z2p, y3p, vd1, vc1, vp1, ring, acc, out_v, load_sem, w2_sem, ring_sem, send_sem, recv_sem):
    r = lax.axis_index("row")
    c = lax.axis_index("col")
    has_up = r > 0
    has_down = r < rows - 1
    images = x_ref.shape[3]
    part = acc.shape[2]

    c1, c2, c3 = wd1.shape[2], wd2.shape[2], wd3.shape[2]

    def ring_view(chunk, base):
        slot, sub = base + chunk // 4, chunk % 4
        return ring.at[slot, pl.ds((sub // 2) * c1, c1), pl.ds((sub % 2) * c2, c2)]

    def ring_block(chunk, base, n0):
        slot, sub = base + chunk // 4, chunk % 4
        return ring[slot, pl.ds((sub // 2) * c1, c1), pl.ds((sub % 2) * c2 + n0, part)]

    load_x = pltpu.make_async_copy(x_ref, xp.at[pl.ds(1, 8), pl.ds(1, x_ref.shape[1])], load_sem.at[0])
    load_d1 = pltpu.make_async_copy(wd1, vd1, load_sem.at[1])
    load_c1 = pltpu.make_async_copy(wc1, vc1, load_sem.at[2])
    load_p1 = pltpu.make_async_copy(wp1, vp1, load_sem.at[3])
    loads_d2 = [pltpu.make_async_copy(wd2.at[t], ring_view(t, 0), w2_sem.at[t]) for t in range(9)]
    loads_d2.append(pltpu.make_async_copy(wp2, ring_view(9, 0), w2_sem.at[9]))
    loads_c2 = [pltpu.make_async_copy(wc2.at[q // 2, pl.ds((q % 2) * c1, c1)], ring_view(q, 3), w2_sem.at[10 + q]) for q in range(18)]

    def group_copy(g):
        kind, ky, kx, kh = GROUPS[g]
        if kind == "down":
            src = wd3.at[ky * 3 + kx]
        elif kind == "proj":
            src = wp3
        else:
            src = wc3.at[ky * 3 + kx, pl.ds(kh * c2, c2)]
        return pltpu.make_async_copy(src, ring.at[g % RING], ring_sem.at[g % RING])

    up, down = jnp.maximum(r - 1, 0), jnp.minimum(r + 1, rows - 1)
    copies = []

    def halo(src, dst, row, col, send_if, recv_if):
        index = len(copies)
        copy = pltpu.make_async_remote_copy(src_ref=src, dst_ref=dst, send_sem=send_sem.at[index], recv_sem=recv_sem.at[index],
                                            device_id={"row": row, "col": col}, device_id_type=pl.DeviceIdType.MESH)
        copies.append((copy, send_if))

        def start():
            if send_if is None:
                copy.start()
            else:
                pl.when(send_if)(copy.start)

        def arrive():
            if recv_if is None:
                copy.wait_recv()
            else:
                pl.when(recv_if)(copy.wait_recv)

        return start, arrive

    is_left = c == 0
    is_right = c == 1
    other = 1 - c

    def pair_row(src_row, buf):
        w = buf.shape[1] - 1
        return halo(src_row, buf.at[0, pl.ds(1, w)], down, c, has_down, has_up)

    def pair_diag(src_pixel, buf):
        return halo(src_pixel, buf.at[0, 0, 1], down, other, has_down & is_left, has_up & is_right)

    def pair_col(src_col, dst_col):
        return halo(src_col, dst_col, r, other, is_left, is_right)

    def plain_row(buf, towards_down):
        n, w = buf.shape[0], buf.shape[1]
        if towards_down:
            return halo(buf.at[n - 2, pl.ds(1, w - 2)], buf.at[0, pl.ds(1, w - 2)], down, c, has_down, has_up)
        return halo(buf.at[1, pl.ds(1, w - 2)], buf.at[n - 1, pl.ds(1, w - 2)], up, c, has_up, has_down)

    def plain_edge(buf):
        w = buf.shape[1]
        return (w - 2) - (w - 3) * c, (w - 1) * c

    def plain_diag(buf, towards_down):
        n = buf.shape[0]
        src_col, dst_col = plain_edge(buf)
        if towards_down:
            return halo(buf.at[n - 2, src_col], buf.at[0, dst_col], down, other, has_down, has_up)
        return halo(buf.at[1, src_col], buf.at[n - 1, dst_col], up, other, has_up, has_down)

    def plain_col(buf, first, count):
        src_col, dst_col = plain_edge(buf)
        return halo(buf.at[pl.ds(first, count), src_col], buf.at[pl.ds(first, count), dst_col], r, other, None, None)

    w1, w2, w3 = y1p.shape[1] - 2, y2p.shape[1] - 2, y3p.shape[1] - 2
    x_row = pair_row(x_ref.at[7], xp)
    x_diag = pair_diag(x_ref.at[7, w1 - 1, 1], xp)
    x_col = pair_col(x_ref.at[pl.ds(0, 8), w1 - 1, 1], xp.at[pl.ds(1, 8), 0, 1])
    y1_down, y1_up = plain_row(y1p, True), plain_row(y1p, False)
    y1_ddown, y1_dup = plain_diag(y1p, True), plain_diag(y1p, False)
    y1_col_b, y1_col_a = plain_col(y1p, 2, 3), plain_col(y1p, 1, 1)
    z1_row = pair_row(z1p.at[4, pl.ds(1, w1 // 2)], z1p)
    z1_diag = pair_diag(z1p.at[4, w1 // 2, 1], z1p)
    z1_cols = [pair_col(z1p.at[pl.ds(a, n), w1 // 2, 1], z1p.at[pl.ds(a, n), 0, 1]) for a, n in ((1, 1), (2, 2), (4, 1))]
    y2_down, y2_up = plain_row(y2p, True), plain_row(y2p, False)
    y2_ddown, y2_dup = plain_diag(y2p, True), plain_diag(y2p, False)
    y2_col_b, y2_col_a = plain_col(y2p, 2, 1), plain_col(y2p, 1, 1)
    z2_row = pair_row(z2p.at[2, pl.ds(1, w2 // 2)], z2p)
    z2_diag = pair_diag(z2p.at[2, w2 // 2, 1], z2p)
    z2_cols = [pair_col(z2p.at[pl.ds(a, 1), w2 // 2, 1], z2p.at[pl.ds(a, 1), 0, 1]) for a in (1, 2)]
    y3_down, y3_up = plain_row(y3p, True), plain_row(y3p, False)
    y3_ddown, y3_dup = plain_diag(y3p, True), plain_diag(y3p, False)
    y3_col = plain_col(y3p, 1, 1)

    def start(*ops):
        for op in ops:
            op[0]()

    def arrive(*ops):
        for op in ops:
            op[1]()

    for buf in (xp, z1p, z2p):
        @pl.when(has_up == False)
        def _(buf=buf):
            buf[0] = jnp.zeros(buf.shape[1:], BF16)

        @pl.when(is_left)
        def _(buf=buf):
            buf[:, 0, 1] = jnp.zeros((buf.shape[0],) + buf.shape[3:], BF16)

    for buf in (y1p, y2p, y3p):
        n, w = buf.shape[0], buf.shape[1]

        @pl.when(has_up == False)
        def _(buf=buf):
            buf[0] = jnp.zeros(buf.shape[1:], BF16)

        @pl.when(has_down == False)
        def _(buf=buf, n=n):
            buf[n - 1] = jnp.zeros(buf.shape[1:], BF16)

        @pl.when(is_left)
        def _(buf=buf):
            buf[:, 0] = jnp.zeros((buf.shape[0],) + buf.shape[2:], BF16)

        @pl.when(is_right)
        def _(buf=buf, w=w):
            buf[:, w - 1] = jnp.zeros((buf.shape[0],) + buf.shape[2:], BF16)

    load_x.start()
    load_d1.start()
    barrier = pltpu.get_barrier_semaphore()

    def signal(row, col):
        pl.semaphore_signal(barrier, inc=1, device_id={"row": row, "col": col}, device_id_type=pl.DeviceIdType.MESH)

    signal(r, other)

    @pl.when(has_up)
    def _():
        signal(up, c)
        signal(up, other)

    @pl.when(has_down)
    def _():
        signal(down, c)
        signal(down, other)

    inner = has_up & has_down

    @pl.when(inner)
    def _():
        pl.semaphore_wait(barrier, 5)

    @pl.when(inner == False)
    def _():
        pl.semaphore_wait(barrier, 3)

    start(x_col, x_diag, x_row)

    def piece(taps, n_all, slot=None, fresh=True, bias=None, store=None):
        for n0 in range(0, n_all, part):
            total = None
            for lhs, weight in taps:
                left = lhs()
                prod = jnp.dot(left, weight(n0), preferred_element_type=F32)
                total = prod if total is None else total + prod
            m = total.shape[0]
            at = pl.ds((n0 // part) * m, m)
            if not fresh:
                total = total + acc[slot, at]
            if store is None:
                acc[slot, at] = total
            else:
                store(n0, jnp.maximum(total + bias[:, pl.ds(n0, part)], 0.0).astype(BF16))

    def pair_lhs(buf, row, kx):
        w = buf.shape[1] - 1
        return lambda: buf[row, pl.ds((kx + 1) // 2, w), (kx + 1) % 2].reshape(w * images, buf.shape[4])

    def plain_lhs(buf, row, kx, k0=0, k=None):
        w = buf.shape[1] - 2
        k = k or buf.shape[3]
        return lambda: buf[row, pl.ds(kx, w), :, pl.ds(k0, k)].reshape(w * images, k)

    def down1(h, kys, **kw):
        def store(n0, value):
            y1p[h + 1, pl.ds(1, w1), :, pl.ds(n0, part)] = value.reshape(w1, images, part)
        taps = [(pair_lhs(xp, 2 * h + ky, kx), lambda n0, t=3 * ky + kx: vd1[t, :, pl.ds(n0, part)]) for ky in kys for kx in range(3)]
        piece(taps, c1, bias=bd1, store=store if kw.pop("final", True) else None, **kw)

    def conv1(h, kys, proj=False, **kw):
        def store(n0, value):
            z1p[h + 1, pl.ds(1, w1 // 2), :, :, pl.ds(n0, part)] = value.reshape(w1 // 2, 2, images, part)
        taps = [(plain_lhs(y1p, h + ky, kx), lambda n0, t=3 * ky + kx: vc1[t, :, pl.ds(n0, part)]) for ky in kys for kx in range(3)]
        if proj:
            taps.append((pair_lhs(xp, 2 * h + 1, 1), lambda n0: vp1[:, pl.ds(n0, part)]))
        piece(taps, c1, bias=bc1, store=store if kw.pop("final", True) else None, **kw)

    def down2(h, kys, **kw):
        def store(n0, value):
            y2p[h + 1, pl.ds(1, w2), :, pl.ds(n0, part)] = value.reshape(w2, images, part)
        taps = [(pair_lhs(z1p, 2 * h + ky, kx), lambda n0, t=3 * ky + kx: ring_block(t, 0, n0)) for ky in kys for kx in range(3)]
        piece(taps, c2, bias=bd2, store=store if kw.pop("final", True) else None, **kw)

    def conv2(h, kys, proj=False, **kw):
        def store(n0, value):
            z2p[h + 1, pl.ds(1, w2 // 2), :, :, pl.ds(n0, part)] = value.reshape(w2 // 2, 2, images, part)
        taps = [(plain_lhs(y2p, h + ky, kx, kh * c1, c1), lambda n0, q=2 * (3 * ky + kx) + kh: ring_block(q, 3, n0))
                for ky in kys for kx in range(3) for kh in range(2)]
        if proj:
            taps.append((pair_lhs(z1p, 2 * h + 1, 1), lambda n0: ring_block(9, 0, n0)))
        piece(taps, c2, bias=bc2, store=store if kw.pop("final", True) else None, **kw)

    m3 = w3 * images

    def group_dots(left, slot, into, fresh=False):
        for n0 in range(0, c3, part):
            at = pl.ds((n0 // part) * m3, m3)
            prod = jnp.dot(left, ring[slot, :, pl.ds(n0, part)], preferred_element_type=F32)
            acc[into, at] = prod if fresh else acc[into, at] + prod

    def stage3_group(g, into, fresh=False):
        kind, ky, kx, kh = GROUPS[g]
        group_copy(g).wait()
        left = pair_lhs(z2p, 1, 1)() if kind == "proj" else pair_lhs(z2p, ky, kx)()
        group_dots(left, g % RING, into, fresh)
        if g + RING < len(GROUPS):
            group_copy(g + RING).start()

    def conv3(ky, first):
        def body(i, carry):
            kx, kh = i // 2, lax.rem(i, 2)
            g = first + i
            slot = lax.rem(g, RING)
            pltpu.make_async_copy(wc3.at[0, pl.ds(0, c2)], ring.at[slot], ring_sem.at[slot]).wait()
            left = y3p[ky, pl.ds(kx, w3), :, pl.ds(pl.multiple_of(kh * c2, c2), c2)].reshape(m3, c2)
            group_dots(left, slot, 1)
            nxt = g + RING - CONV_0

            @pl.when(g + RING < len(GROUPS))
            def _():
                nky = jnp.where(nxt < 12, 0, 2)
                tap = 3 * nky + lax.rem(nxt, 6) // 2
                k0 = pl.multiple_of(lax.rem(nxt, 2) * c2, c2)
                pltpu.make_async_copy(wc3.at[tap, pl.ds(k0, c2)], ring.at[slot], ring_sem.at[slot]).start()
            return carry
        lax.fori_loop(0, 6, body, 0)

    load_x.wait()
    load_d1.wait()
    load_c1.start()
    load_p1.start()
    arrive(x_col)
    down1(3, (0, 1, 2))
    start(y1_ddown, y1_down)
    for copy in loads_d2:
        copy.start()
    down1(1, (0, 1, 2))
    down1(2, (0, 1, 2))
    start(y1_col_b)
    for copy in loads_c2:
        copy.start()
    down1(0, (1, 2), slot=0, final=False)
    load_c1.wait()
    load_p1.wait()
    arrive(y1_col_b)
    conv1(2, (0, 1, 2), proj=True)
    conv1(1, (1, 2), proj=True, slot=1, final=False)
    conv1(3, (0, 1), proj=True, slot=2, final=False)
    arrive(x_row, x_diag)
    down1(0, (0,), slot=0, fresh=False)
    start(y1_col_a, y1_dup, y1_up)
    arrive(y1_col_a)
    conv1(1, (0,), slot=1, fresh=False)
    start(z1_cols[1])
    conv1(0, (1, 2), proj=True, slot=0, final=False)
    for copy in loads_d2:
        copy.wait()
    arrive(z1_cols[1])
    down2(1, (0, 1), slot=1, final=False)
    arrive(y1_down, y1_ddown)
    conv1(0, (0,), slot=0, fresh=False)
    start(z1_cols[0])
    arrive(y1_up, y1_dup)
    conv1(3, (2,), slot=2, fresh=False)
    start(z1_cols[2], z1_diag, z1_row)

    arrive(z1_cols[2])
    down2(1, (2,), slot=1, fresh=False)
    start(y2_col_b, y2_ddown, y2_down)
    arrive(z1_cols[0])
    down2(0, (1, 2), slot=0, final=False)
    for copy in loads_c2:
        copy.wait()
    arrive(y2_col_b)
    conv2(1, (1,), proj=True, slot=1, final=False)
    conv2(0, (2,), proj=True, slot=2, final=False)
    arrive(z1_row, z1_diag)
    down2(0, (0,), slot=0, fresh=False)
    start(y2_col_a, y2_dup, y2_up)
    for g in range(3):
        group_copy(g).start()
    arrive(y2_col_a)
    conv2(1, (0,), slot=1, fresh=False, final=False)
    conv2(0, (1,), slot=2, fresh=False, final=False)
    arrive(y2_up, y2_dup)
    conv2(1, (2,), slot=1, fresh=False)
    start(z2_cols[1], z2_diag, z2_row)
    arrive(y2_down, y2_ddown)
    conv2(0, (0,), slot=2, fresh=False)
    start(z2_cols[0])
    for g in range(3, RING):
        group_copy(g).start()

    arrive(z2_cols[1])
    for g in range(3):
        stage3_group(g, 0, fresh=g == 0)
    arrive(z2_cols[0])
    for g in range(3, 6):
        stage3_group(g, 0)
    stage3_group(6, 1, fresh=True)
    arrive(z2_row, z2_diag)
    for g in range(7, 10):
        stage3_group(g, 0)
    for n0 in range(0, c3, part):
        total = acc[0, pl.ds((n0 // part) * m3, m3)] + bd3[:, pl.ds(n0, part)]
        y3p[1, pl.ds(1, w3), :, pl.ds(n0, part)] = jnp.maximum(total, 0.0).astype(BF16).reshape(w3, images, part)
    start(y3_col, y3_ddown, y3_dup, y3_down, y3_up)
    arrive(y3_col)
    conv3(1, CONV_0)
    arrive(y3_down, y3_ddown)
    conv3(0, CONV_0 + 6)
    arrive(y3_up, y3_dup)
    conv3(2, CONV_0 + 12)
    for n0 in range(0, c3, part):
        total = acc[1, pl.ds((n0 // part) * m3, m3)] + bc3[:, pl.ds(n0, part)]
        out_v[:, :, pl.ds(n0, part)] = jnp.maximum(total, 0.0).astype(BF16).reshape(w3, images, part)
    put = pltpu.make_async_copy(out_v, out_ref, load_sem.at[0])
    put.start()
    for copy, send_if in copies:
        if send_if is None:
            copy.wait_send()
        else:
            pl.when(send_if)(copy.wait_send)
    put.wait()


def solution(mesh):
    row_count = mesh.shape["row"]
    col_count = mesh.shape["col"]
    tile_spec = P("batch", "row", "col")

    def local_blocks(x_tile, *params):
        images, tile_h, tile_w, c0 = x_tile.shape
        x_in = x_tile.transpose(1, 2, 0, 3).reshape(tile_h, tile_w // 2, 2, images, c0)
        weights, biases = [], []
        for stage in range(3):
            w_down, b_down, w_conv, b_conv, w_proj = params[5 * stage:5 * stage + 5]
            weights += [w_down.reshape((9,) + w_down.shape[2:]), w_conv.reshape((9,) + w_conv.shape[2:]), w_proj]
            biases += [b_down.reshape(1, -1), b_conv.reshape(1, -1)]
        c1, c2, c3 = (weights[3 * stage].shape[2] for stage in range(3))
        w1, w2, w3 = tile_w // 2, tile_w // 4, tile_w // 8
        any_spec = pl.BlockSpec(memory_space=pl.ANY)
        vmem_spec = pl.BlockSpec(memory_space=pltpu.VMEM)
        copy_count = 29
        out = pl.pallas_call(
            lambda *refs: encoder_kernel(row_count, col_count, *refs),
            out_shape=jax.ShapeDtypeStruct((w3, images, c3), BF16),
            in_specs=[any_spec] * 10 + [vmem_spec] * 6,
            out_specs=any_spec,
            scratch_shapes=[
                pltpu.VMEM((tile_h + 1, w1 + 1, 2, images, c0), BF16),
                pltpu.VMEM((6, w1 + 2, images, c1), BF16),
                pltpu.VMEM((5, w2 + 1, 2, images, c1), BF16),
                pltpu.VMEM((4, w2 + 2, images, c2), BF16),
                pltpu.VMEM((3, w3 + 1, 2, images, c2), BF16),
                pltpu.VMEM((3, w3 + 2, images, c3), BF16),
                pltpu.VMEM((9, c0, c1), BF16),
                pltpu.VMEM((9, c1, c1), BF16),
                pltpu.VMEM((c0, c1), BF16),
                pltpu.VMEM((RING, c2, c3), BF16),
                pltpu.VMEM((3, w1 * images, c1), F32),
                pltpu.VMEM((w3, images, c3), BF16),
                pltpu.SemaphoreType.DMA((4,)),
                pltpu.SemaphoreType.DMA((28,)),
                pltpu.SemaphoreType.DMA((RING,)),
                pltpu.SemaphoreType.DMA((copy_count,)),
                pltpu.SemaphoreType.DMA((copy_count,)),
            ],
            compiler_params=pltpu.CompilerParams(collective_id=0, has_side_effects=True, vmem_limit_bytes=67043328),
            name="encoder",
        )(x_in, *weights, *biases)
        return out.transpose(1, 0, 2).reshape(images, 1, w3, c3)

    return jax.shard_map(local_blocks, mesh=mesh, in_specs=(tile_spec,) + (P(),) * 15, out_specs=tile_spec, check_vma=False)
```

```python
import jax
import jax.numpy as jnp
import numpy as np
from jax import lax
from jax.experimental import pallas as pl
from jax.experimental.pallas import tpu as pltpu
from jax.sharding import PartitionSpec as P

F32 = jnp.float32
BF16 = jnp.bfloat16
RING = 10
RAW = 4
TAPS = (0, 1, 2)
MID = dict(final=False)
END = dict(fresh=False)
PROJ = dict(proj=True)


def encoder_kernel(rows, cols, x_ref, wd1, wc1, wp1, wd2, wc2, wp2, wd3, wc3, wp3, bd1, bc1, bd2, bc2, bd3, bc3, perm, out_ref,
                   xp, y1p, z1p, y2p, z2p, y3p, ring, acc, out_v, raw, raw_halo, out_sem, raw_sem, w1_sem, w2_sem, ring_sem, send_sem, recv_sem):
    r = lax.axis_index("row")
    c = lax.axis_index("col")
    has_up = r > 0
    has_down = r < rows - 1
    images = x_ref.shape[0]
    part = acc.shape[2]
    c0, c1, c2, c3 = x_ref.shape[3], wd1.shape[2], wd2.shape[2], wd3.shape[2]

    def place_c1(t):
        if t == 8:
            return 9, 0, 0
        return 8, (t // 4) * c1, (t % 4) * c1

    def place_d1(t):
        return 9, (t % 4) * c0, (1 + t // 4) * c1

    def place_d2(t):
        q = (t - 3 if t < 9 else 6) if t > 2 else 8 + t
        return q // 4, ((q % 4) // 2) * c1, (q % 2) * c2

    def place_c2(tap, kh):
        q = 2 * ((tap + 6) % 9) + kh
        return 3 + q // 4, ((q % 4) // 2) * c1, (q % 2) * c2

    def load(src, place, size, sem):
        slot, k0, n0 = place
        return pltpu.make_async_copy(src, ring.at[slot, pl.ds(k0, size[0]), pl.ds(n0, size[1])], sem)

    def block(place, k, n0):
        slot, k0, n1 = place
        return ring[slot, pl.ds(k0, k), pl.ds(n1 + n0, part)]

    loads_d1 = [load(wd1.at[t], place_d1(t), (c0, c1), w1_sem.at[t]) for t in range(9)]
    loads_d1.append(load(wp1, place_d1(9), (c0, c1), w1_sem.at[9]))
    loads_c1 = [load(wc1.at[t], place_c1(t), (c1, c1), w1_sem.at[10 + t]) for t in range(9)]
    loads_d2 = [load(wd2.at[t], place_d2(t), (c1, c2), w2_sem.at[t]) for t in range(9)]
    loads_d2.append(load(wp2, place_d2(9), (c1, c2), w2_sem.at[9]))
    loads_c2 = [load(wc2.at[q // 2, pl.ds((q % 2) * c1, c1)], place_c2(q // 2, q % 2), (c1, c2), w2_sem.at[10 + q]) for q in range(18)]

    def first_groups(g):
        if g == 6:
            src = wp3
        else:
            ky = 2 if g < 3 else 1 if g < 6 else 0
            kx = g % 3 if g < 6 else g - 7
            src = wd3.at[3 * ky + kx]
        return pltpu.make_async_copy(src, ring.at[(g + 8) % RING], ring_sem.at[(g + 8) % RING])

    def conv3_copy(tap, k0, slot):
        return pltpu.make_async_copy(wc3.at[tap, pl.ds(k0, c2)], ring.at[slot], ring_sem.at[slot])

    def conv3_first(j):
        if j < 6:
            tap, kh = 3 + j // 2, j % 2
        else:
            tap, kh = 6 * ((j - 6) // 3) + (j - 6) % 3, 0
        conv3_copy(tap, kh * c2, (j + 8) % RING).start()

    def group_wait(slot):
        pltpu.make_async_copy(wc3.at[0, pl.ds(0, c2)], ring.at[slot], ring_sem.at[slot]).wait()

    up, down = jnp.maximum(r - 1, 0), jnp.minimum(r + 1, rows - 1)
    copies = []

    def halo(src, dst, row, col, send_if, recv_if):
        index = len(copies)
        copy = pltpu.make_async_remote_copy(src_ref=src, dst_ref=dst, send_sem=send_sem.at[index], recv_sem=recv_sem.at[index],
                                            device_id={"row": row, "col": col}, device_id_type=pl.DeviceIdType.MESH)
        copies.append((send_if, copy.wait_send))
        return copy, send_if, recv_if

    is_left = c == 0
    is_right = c == 1
    up_left, up_right, down_left, down_right = has_up & is_left, has_up & is_right, has_down & is_left, has_down & is_right
    other = 1 - c

    w1, w2, w3 = y1p.shape[1] - 2, y2p.shape[1] - 2, y3p.shape[1] - 2

    def parts(w, a):
        return (0, a), (a, w - a)

    y1_parts = parts(w1, w2 + 3)
    z1_parts = parts(w1, w2 + 2)
    y2_parts = parts(w2, w3 + 1)
    z2_parts = parts(w2, w3)

    def pair_rows(buf, sections):
        n = buf.shape[0]
        ops = []
        for first, count in sections:
            cells = pl.ds(1 + first // 2, count // 2)
            ops.append(halo(buf.at[n - 1, cells], buf.at[0, cells], down, c, has_down, has_up))
        return ops

    def pair_diag(buf):
        n, w = buf.shape[0], buf.shape[1] - 1
        return halo(buf.at[n - 1, w, 1], buf.at[0, 0, 1], down, other, down_left, up_right)

    def pair_col(buf, first, count):
        w = buf.shape[1] - 1
        return halo(buf.at[pl.ds(first, count), w, 1], buf.at[pl.ds(first, count), 0, 1], r, other, is_left, is_right)

    def plain_down(buf, k0=0, k=None):
        n, w, k = buf.shape[0], buf.shape[1], k or buf.shape[3]
        at = (pl.ds(1, w - 2), pl.ds(0, images), pl.ds(k0, k))
        return halo(buf.at[(n - 2,) + at], buf.at[(0,) + at], down, c, has_down, has_up)

    def plain_ups(buf, sections, k0=0, k=None):
        n, k = buf.shape[0], k or buf.shape[3]
        ops = []
        for first, count in sections:
            at = (pl.ds(1 + first, count), pl.ds(0, images), pl.ds(k0, k))
            ops.append(halo(buf.at[(1,) + at], buf.at[(n - 1,) + at], up, c, has_up, has_down))
        return ops

    def plain_edge(buf):
        w = buf.shape[1]
        return (w - 2) - (w - 3) * c, (w - 1) * c

    def plain_diag(buf, towards_down, k0=0, k=None):
        n, k = buf.shape[0], k or buf.shape[3]
        src_col, dst_col = plain_edge(buf)
        at = (pl.ds(0, images), pl.ds(k0, k))
        if towards_down:
            return halo(buf.at[(n - 2, src_col) + at], buf.at[(0, dst_col) + at], down, other, has_down, has_up)
        return halo(buf.at[(1, src_col) + at], buf.at[(n - 1, dst_col) + at], up, other, has_up, has_down)

    def plain_col(buf, first, count, k0=0, k=None):
        k = k or buf.shape[3]
        src_col, dst_col = plain_edge(buf)
        at = (pl.ds(0, images), pl.ds(k0, k))
        return halo(buf.at[(pl.ds(first, count), src_col) + at], buf.at[(pl.ds(first, count), dst_col) + at], r, other, None, None)

    x_row = halo(x_ref.at[:, 7], raw_halo, down, c, has_down, has_up)
    x_diag = pair_diag(xp)
    x_col_b, x_col_a = pair_col(xp, 6, 3), pair_col(xp, 1, 5)
    y1_down, y1_ups = plain_down(y1p), plain_ups(y1p, y1_parts)
    y1_ddown, y1_dup = plain_diag(y1p, True), plain_diag(y1p, False)
    y1_col_b, y1_col_a = plain_col(y1p, 2, 3), plain_col(y1p, 1, 1)
    z1_rows, z1_diag = pair_rows(z1p, z1_parts), pair_diag(z1p)
    z1_cols = [pair_col(z1p, a, n) for a, n in ((1, 1), (2, 2), (4, 1))]
    y2_down, y2_ups = plain_down(y2p), plain_ups(y2p, y2_parts)
    y2_ddown, y2_dup = plain_diag(y2p, True), plain_diag(y2p, False)
    y2_col_b, y2_col_a = plain_col(y2p, 2, 1), plain_col(y2p, 1, 1)
    z2_rows, z2_diag = pair_rows(z2p, z2_parts), pair_diag(z2p)
    z2_cols = [pair_col(z2p, a, 1) for a in (1, 2)]
    y3_halves = []
    for k0 in (0, c2):
        y3_halves.append((plain_col(y3p, 1, 1, k0, c2), plain_diag(y3p, True, k0, c2), plain_diag(y3p, False, k0, c2),
                          plain_down(y3p, k0, c2), plain_ups(y3p, ((0, w3),), k0, c2)[0]))

    def under_conditions(items):
        groups = {}
        for condition, action in items:
            groups.setdefault(id(condition), (condition, []))[1].append(action)
        for condition, actions in groups.values():
            def run(actions=actions):
                for action in actions:
                    action()
            if condition is None:
                run()
            else:
                pl.when(condition)(run)

    def start(*ops):
        under_conditions([(send_if, copy.start) for copy, send_if, _ in ops])

    def arrive(*ops):
        under_conditions([(recv_if, copy.wait_recv) for copy, _, recv_if in ops])

    def start_with_diag(row, diag, last):
        under_conditions([(has_up, row[0].start), (up_left if last else up_right, diag[0].start)])

    def arrive_with_diag(row, diag, last):
        under_conditions([(has_down, row[0].wait_recv), (down_left if last else down_right, diag[0].wait_recv)])

    pair_bufs, plain_bufs = (xp, z1p, z2p), (y1p, y2p, y3p)

    @pl.when(has_up == False)
    def _():
        raw_halo[...] = jnp.zeros(raw_halo.shape, BF16)
        for buf in pair_bufs + plain_bufs:
            buf[0] = jnp.zeros(buf.shape[1:], BF16)

    @pl.when(has_down == False)
    def _():
        for buf in plain_bufs:
            buf[buf.shape[0] - 1] = jnp.zeros(buf.shape[1:], BF16)

    @pl.when(is_left)
    def _():
        for buf in pair_bufs:
            buf[:, 0, 1] = jnp.zeros((buf.shape[0],) + buf.shape[3:], BF16)
        for buf in plain_bufs:
            buf[:, 0] = jnp.zeros((buf.shape[0],) + buf.shape[2:], BF16)

    @pl.when(is_right)
    def _():
        for buf in plain_bufs:
            buf[:, buf.shape[1] - 1] = jnp.zeros((buf.shape[0],) + buf.shape[2:], BF16)

    def raw_copy(h):
        slot = h % RAW
        return pltpu.make_async_copy(x_ref.at[:, h], raw.at[slot], raw_sem.at[slot])

    for h in range(7, 7 - RAW, -1):
        raw_copy(h).start()
    for copy in loads_d1:
        copy.start()
    barrier = pltpu.get_barrier_semaphore()

    def signal(row, col):
        pl.semaphore_signal(barrier, inc=1, device_id={"row": row, "col": col}, device_id_type=pl.DeviceIdType.MESH)

    signal(r, other)

    @pl.when(has_up)
    def _():
        signal(up, c)
        signal(up, other)

    @pl.when(has_down)
    def _():
        signal(down, c)
        signal(down, other)

    inner = has_up & has_down

    @pl.when(inner)
    def _():
        pl.semaphore_wait(barrier, 5)

    @pl.when(inner == False)
    def _():
        pl.semaphore_wait(barrier, 3)

    start(x_row)

    size = images * images

    def turn(src, index, row, b):
        at = pl.ds(b * images if isinstance(b, int) else pl.multiple_of(b * images, images), images)
        value = jnp.dot(perm[...], src[index + (slice(None), at)].reshape(size, c0), preferred_element_type=F32)
        xp[row, pl.ds(1 + b * (images // 2), images // 2)] = value.astype(BF16).reshape(images // 2, 2, images, c0)

    blocks = 2 * w1 // images

    def turn_rows(first, count):
        for h in range(first, first - count, -1):
            raw_copy(h).wait()
            for b in range(blocks):
                turn(raw, (h % RAW,), h + 1, b)
            if h >= RAW:
                raw_copy(h - RAW).start()

    def piece(taps, n_all, w, section, slot=None, fresh=True, bias=None, store=None):
        first, count = section
        for n0 in range(0, n_all, part):
            total = None
            for lhs, weight in taps:
                prod = jnp.dot(lhs(first, count), weight(n0), preferred_element_type=F32)
                total = prod if total is None else total + prod
            at = pl.ds((n0 // part) * w * images + first * images, count * images)
            if not fresh:
                total = total + acc[slot, at]
            if store is None:
                acc[slot, at] = total
            else:
                store(n0, jnp.maximum(total + bias[:, pl.ds(n0, part)], 0.0).astype(BF16), first, count)

    def pair_lhs(buf, row, kx):
        return lambda first, count: buf[row, pl.ds(first + (kx + 1) // 2, count), (kx + 1) % 2].reshape(count * images, buf.shape[4])

    def plain_lhs(buf, row, kx, k0=0, k=None):
        k = k or buf.shape[3]
        return lambda first, count: buf[row, pl.ds(first + kx, count), :, pl.ds(k0, k)].reshape(count * images, k)

    def plain_store(buf, h):
        def store(n0, value, first, count):
            buf[h + 1, pl.ds(1 + first, count), :, pl.ds(n0, part)] = value.reshape(count, images, part)
        return store

    def pair_store(buf, h):
        def store(n0, value, first, count):
            buf[h + 1, pl.ds(1 + first // 2, count // 2), :, :, pl.ds(n0, part)] = value.reshape(count // 2, 2, images, part)
        return store

    def down1(h, kys, section=(0, w1), final=True, **kw):
        taps = [(pair_lhs(xp, 2 * h + ky, kx), lambda n0, t=3 * ky + kx: block(place_d1(t), c0, n0)) for ky in kys for kx in TAPS]
        piece(taps, c1, w1, section, bias=bd1, store=plain_store(y1p, h) if final else None, **kw)

    def conv1(h, kys, section=(0, w1), final=True, proj=False, **kw):
        taps = [(plain_lhs(y1p, h + ky, kx), lambda n0, t=3 * ky + kx: block(place_c1(t), c1, n0)) for ky in kys for kx in TAPS]
        if proj:
            taps.append((pair_lhs(xp, 2 * h + 1, 1), lambda n0: block(place_d1(9), c0, n0)))
        piece(taps, c1, w1, section, bias=bc1, store=pair_store(z1p, h) if final else None, **kw)

    def down2(h, kys, section=(0, w2), final=True, **kw):
        taps = [(pair_lhs(z1p, 2 * h + ky, kx), lambda n0, t=3 * ky + kx: block(place_d2(t), c1, n0)) for ky in kys for kx in TAPS]
        piece(taps, c2, w2, section, bias=bd2, store=plain_store(y2p, h) if final else None, **kw)

    def conv2(h, kys, section=(0, w2), final=True, proj=False, **kw):
        taps = [(plain_lhs(y2p, h + ky, kx, kh * c1, c1), lambda n0, t=3 * ky + kx, kh=kh: block(place_c2(t, kh), c1, n0))
                for ky in kys for kx in TAPS for kh in range(2)]
        if proj:
            taps.append((pair_lhs(z1p, 2 * h + 1, 1), lambda n0: block(place_d2(9), c1, n0)))
        piece(taps, c2, w2, section, bias=bc2, store=pair_store(z2p, h) if final else None, **kw)

    m3 = w3 * images

    def group_dots(left, slot, into, fresh=False, n_range=None):
        for n0 in range(*(n_range or (0, c3)), part):
            at = pl.ds((n0 // part) * m3, m3)
            prod = jnp.dot(left, ring[slot, :, pl.ds(n0, part)], preferred_element_type=F32)
            acc[into, at] = prod if fresh else acc[into, at] + prod

    def z2_left(row, kx):
        return z2p[row, pl.ds((kx + 1) // 2, w3), (kx + 1) % 2].reshape(m3, c2)

    def down3(ky, g0):
        for kx in TAPS:
            slot = (g0 + kx + 8) % RING
            first_groups(g0 + kx).wait()
            group_dots(z2_left(ky, kx), slot, 0, fresh=g0 + kx == 0)
            conv3_first(g0 + kx)

    def conv3(first):
        def body(i, carry):
            slot = lax.rem(i + first + 8, RING)
            group_wait(slot)
            if first == 0:
                ky, kx, k0 = 1, i // 2, pl.multiple_of(lax.rem(i, 2) * c2, c2)
            else:
                ky, kx, k0 = 2 * (i // 3), lax.rem(i, 3), (first // 6 - 1) * c2
            left = y3p[ky, pl.ds(kx, w3), :, pl.ds(k0, c2)].reshape(m3, c2)
            group_dots(left, slot, 1)
            if first == 0:
                later = lax.rem(i + 4, 6)
                conv3_copy(6 * (later // 3) + lax.rem(later, 3), pl.multiple_of((i + 4) // 6 * c2, c2), slot).start()
            elif first == 6:
                @pl.when(i < 2)
                def _():
                    conv3_copy(7 + i, c2, slot).start()
            return carry
        lax.fori_loop(0, 6, body, 0)

    turn_rows(7, 3)
    start(x_col_b, x_diag)
    for copy in loads_c1:
        copy.start()
    turn_rows(4, 2)
    for copy in loads_d1:
        copy.wait()
    arrive(x_col_b)
    down1(3, TAPS)
    start(y1_ddown, y1_down)
    for copy in loads_d2:
        copy.start()
    turn_rows(2, 3)
    start(x_col_a)
    for copy in loads_c2:
        copy.start()
    arrive(x_col_a)
    down1(1, TAPS)
    down1(2, TAPS)
    start(y1_col_b)
    down1(0, TAPS[1:], slot=0, **MID)
    for copy in loads_c1:
        copy.wait()
    arrive(y1_col_b)
    conv1(2, TAPS, **PROJ)
    conv1(1, TAPS[1:], **PROJ, slot=1, **MID)
    conv1(3, TAPS[:2], **PROJ, slot=2, **MID)
    arrive(x_row, x_diag)
    for b in range(blocks):
        turn(raw_halo, (), 0, b)
    for i, section in enumerate(y1_parts):
        down1(0, TAPS[:1], section, slot=0, **END)
        start_with_diag(y1_ups[i], y1_dup, i)
    start(y1_col_a)
    arrive(y1_col_a)
    conv1(1, TAPS[:1], slot=1, **END)
    start(z1_cols[1])
    conv1(0, TAPS[1:], **PROJ, slot=0, **MID)
    for copy in loads_d2:
        copy.wait()
    arrive(z1_cols[1])
    down2(1, TAPS[:2], slot=1, **MID)
    for i, section in enumerate(z1_parts):
        arrive_with_diag(y1_ups[i], y1_dup, i)
        conv1(3, TAPS[2:], section, slot=2, **END)
        start(z1_rows[i])
    start(z1_cols[2], z1_diag)
    arrive(y1_down, y1_ddown)
    conv1(0, TAPS[:1], slot=0, **END)
    start(z1_cols[0])
    for g in range(2):
        first_groups(g).start()

    arrive(z1_cols[2])
    down2(1, TAPS[2:], slot=1, **END)
    start(y2_col_b, y2_ddown, y2_down)
    arrive(z1_cols[0])
    down2(0, TAPS[1:], slot=0, **MID)
    for copy in loads_c2:
        copy.wait()
    arrive(y2_col_b)
    conv2(1, TAPS[1:2], **PROJ, slot=1, **MID)
    conv2(0, TAPS[2:], **PROJ, slot=2, **MID)
    for g in (2, 3):
        first_groups(g).start()
    arrive(z1_diag)
    for i, section in enumerate(y2_parts):
        arrive(z1_rows[i])
        down2(0, TAPS[:1], section, slot=0, **END)
        start_with_diag(y2_ups[i], y2_dup, i)
    start(y2_col_a)
    first_groups(4).start()
    arrive(y2_col_a)
    conv2(1, TAPS[:1], slot=1, **END, **MID)
    conv2(0, TAPS[1:2], slot=2, **END, **MID)
    first_groups(5).start()
    for i, section in enumerate(z2_parts):
        arrive_with_diag(y2_ups[i], y2_dup, i)
        conv2(1, TAPS[2:], section, slot=1, **END)
        start(z2_rows[i])
    start(z2_cols[1], z2_diag)
    for g in (6, 7):
        first_groups(g).start()
    arrive(y2_down, y2_ddown)
    conv2(0, TAPS[:1], slot=2, **END)
    start(z2_cols[0])
    for g in (8, 9):
        first_groups(g).start()

    arrive(z2_cols[1])
    down3(2, 0)
    arrive(z2_cols[0])
    down3(1, 3)
    first_groups(6).wait()
    group_dots(z2_left(1, 1), (6 + 8) % RING, 1, fresh=True)
    conv3_first(6)
    arrive(*z2_rows, z2_diag)
    for g in range(7, 10):
        first_groups(g).wait()
    for half in range(2):
        for kx in TAPS:
            group_dots(z2_left(0, kx), (kx + 7 + 8) % RING, 0, n_range=(half * c2, half * c2 + c2))
        for n0 in range(half * c2, half * c2 + c2, part):
            total = acc[0, pl.ds((n0 // part) * m3, m3)] + bd3[:, pl.ds(n0, part)]
            y3p[1, pl.ds(1, w3), :, pl.ds(n0, part)] = jnp.maximum(total, 0.0).astype(BF16).reshape(w3, images, part)
        start(*y3_halves[half])
    for j in range(7, 10):
        conv3_first(j)
    arrive(y3_halves[0][0], y3_halves[1][0])
    conv3(0)
    arrive(*y3_halves[0][1:])
    conv3(6)
    arrive(*y3_halves[1][1:])
    conv3(12)
    for n0 in range(0, c3, part):
        total = acc[1, pl.ds((n0 // part) * m3, m3)] + bc3[:, pl.ds(n0, part)]
        out_v[:, :, pl.ds(n0, part)] = jnp.maximum(total, 0.0).astype(BF16).reshape(w3, images, part)
    put = pltpu.make_async_copy(out_v, out_ref, out_sem.at[0])
    put.start()
    under_conditions(copies)
    put.wait()


def solution(mesh):
    row_count = mesh.shape["row"]
    col_count = mesh.shape["col"]
    tile_spec = P("batch", "row", "col")

    def local_blocks(x_tile, *params):
        images, tile_h, tile_w, c0 = x_tile.shape
        weights, biases = [], []
        for stage in TAPS:
            w_down, b_down, w_conv, b_conv, w_proj = params[5 * stage:5 * stage + 5]
            weights += [w_down.reshape((9,) + w_down.shape[2:]), w_conv.reshape((9,) + w_conv.shape[2:]), w_proj]
            biases += [b_down.reshape(1, -1), b_conv.reshape(1, -1)]
        c1, c2, c3 = (weights[3 * stage].shape[2] for stage in TAPS)
        w1, w2, w3 = tile_w // 2, tile_w // 4, tile_w // 8
        any_spec = pl.BlockSpec(memory_space=pl.ANY)
        vmem_spec = pl.BlockSpec(memory_space=pltpu.VMEM)
        index = np.arange(images * images)
        perm = jnp.asarray(index[:, None] == (index % images * images + index // images)[None, :], BF16)
        copy_count = 39
        out = pl.pallas_call(
            lambda *refs: encoder_kernel(row_count, col_count, *refs),
            out_shape=jax.ShapeDtypeStruct((w3, images, c3), BF16),
            in_specs=[any_spec] * 10 + [vmem_spec] * 7,
            out_specs=any_spec,
            scratch_shapes=[
                pltpu.VMEM((tile_h + 1, w1 + 1, 2, images, c0), BF16),
                pltpu.VMEM((6, w1 + 2, images, c1), BF16),
                pltpu.VMEM((5, w2 + 1, 2, images, c1), BF16),
                pltpu.VMEM((4, w2 + 2, images, c2), BF16),
                pltpu.VMEM((3, w3 + 1, 2, images, c2), BF16),
                pltpu.VMEM((3, w3 + 2, images, c3), BF16),
                pltpu.VMEM((RING, c2, c3), BF16),
                pltpu.VMEM((3, w1 * images, c1), F32),
                pltpu.VMEM((w3, images, c3), BF16),
                pltpu.VMEM((RAW, images, tile_w, c0), BF16),
                pltpu.VMEM((images, tile_w, c0), BF16),
                pltpu.SemaphoreType.DMA(TAPS[1:2]),
                pltpu.SemaphoreType.DMA((RAW,)),
                pltpu.SemaphoreType.DMA((19,)),
                pltpu.SemaphoreType.DMA((28,)),
                pltpu.SemaphoreType.DMA((RING,)),
                pltpu.SemaphoreType.DMA((copy_count,)),
                pltpu.SemaphoreType.DMA((copy_count,)),
            ],
            compiler_params=pltpu.CompilerParams(collective_id=0, has_side_effects=True, vmem_limit_bytes=67043328),
            name="encoder",
        )(x_tile, *weights, *biases, perm)
        return out.transpose(1, 0, 2).reshape(images, 1, w3, c3)

    return jax.shard_map(local_blocks, mesh=mesh, in_specs=(tile_spec,) + (P(),) * 15, out_specs=tile_spec, check_vma=False)
```

```python
import jax
import jax.numpy as jnp
import numpy as np
from jax import lax
from jax.experimental import pallas as pl
from jax.experimental.pallas import tpu as pltpu
from jax.sharding import PartitionSpec as P

F32 = jnp.float32
BF16 = jnp.bfloat16
RING = 10
RAW = 4
TAPS = (0, 1, 2)
MID = dict(final=False)
END = dict(fresh=False)
PROJ = dict(proj=True)


def encoder_kernel(rows, cols, x_ref, wd1, wc1, wp1, wd2, wc2, wp2, wd3, wc3, wp3, bd1, bc1, bd2, bc2, bd3, bc3, perm, out_ref,
                   xp, y1p, z1p, y2p, z2p, y3p, ring, acc, out_v, raw, raw_halo, out_sem, raw_sem, w1_sem, w2_sem, ring_sem, send_sem, recv_sem):
    r = lax.axis_index("row")
    c = lax.axis_index("col")
    has_up = r > 0
    has_down = r < rows - 1
    images = x_ref.shape[0]
    part = acc.shape[2]
    c0, c1, c2, c3 = x_ref.shape[4], wd1.shape[2], wd2.shape[2], wd3.shape[2]

    def place_c1(t):
        if t == 8:
            return 9, 0, 0
        return 8, (t // 4) * c1, (t % 4) * c1

    def place_d1(t):
        return 9, (t % 4) * c0, (1 + t // 4) * c1

    def place_d2(t):
        q = (t - 3 if t < 9 else 6) if t > 2 else 8 + t
        return q // 4, ((q % 4) // 2) * c1, (q % 2) * c2

    def place_c2(tap, kh):
        q = 2 * ((tap + 6) % 9) + kh
        return 3 + q // 4, ((q % 4) // 2) * c1, (q % 2) * c2

    def load(src, place, size, sem):
        slot, k0, n0 = place
        return pltpu.make_async_copy(src, ring.at[slot, pl.ds(k0, size[0]), pl.ds(n0, size[1])], sem)

    def block(place, k, n0):
        slot, k0, n1 = place
        return ring[slot, pl.ds(k0, k), pl.ds(n1 + n0, part)]

    loads_d1 = [load(wd1.at[t], place_d1(t), (c0, c1), w1_sem.at[t]) for t in range(9)]
    loads_d1.append(load(wp1, place_d1(9), (c0, c1), w1_sem.at[9]))
    loads_c1 = [load(wc1.at[t], place_c1(t), (c1, c1), w1_sem.at[10 + t]) for t in range(9)]
    loads_d2 = [load(wd2.at[t], place_d2(t), (c1, c2), w2_sem.at[t]) for t in range(9)]
    loads_d2.append(load(wp2, place_d2(9), (c1, c2), w2_sem.at[9]))
    loads_c2 = [load(wc2.at[q // 2, pl.ds((q % 2) * c1, c1)], place_c2(q // 2, q % 2), (c1, c2), w2_sem.at[10 + q]) for q in range(18)]

    def first_groups(g):
        if g == 6:
            src = wp3
        else:
            ky = 2 if g < 3 else 1 if g < 6 else 0
            kx = g % 3 if g < 6 else g - 7
            src = wd3.at[3 * ky + kx]
        return pltpu.make_async_copy(src, ring.at[(g + 8) % RING], ring_sem.at[(g + 8) % RING])

    def conv3_copy(tap, k0, slot):
        return pltpu.make_async_copy(wc3.at[tap, pl.ds(k0, c2)], ring.at[slot], ring_sem.at[slot])

    def conv3_first(j):
        if j < 6:
            tap, kh = 3 + j // 2, j % 2
        else:
            tap, kh = 6 * ((j - 6) // 3) + (j - 6) % 3, 0
        conv3_copy(tap, kh * c2, (j + 8) % RING).start()

    def group_wait(slot):
        pltpu.make_async_copy(wc3.at[0, pl.ds(0, c2)], ring.at[slot], ring_sem.at[slot]).wait()

    up, down = jnp.maximum(r - 1, 0), jnp.minimum(r + 1, rows - 1)
    copies = []

    def halo(src, dst, row, col, send_if, recv_if):
        index = len(copies)
        copy = pltpu.make_async_remote_copy(src_ref=src, dst_ref=dst, send_sem=send_sem.at[index], recv_sem=recv_sem.at[index],
                                            device_id={"row": row, "col": col}, device_id_type=pl.DeviceIdType.MESH)
        copies.append((send_if, copy.wait_send))
        return copy, send_if, recv_if

    is_left = c == 0
    is_right = c == 1
    up_left, up_right, down_left, down_right = has_up & is_left, has_up & is_right, has_down & is_left, has_down & is_right
    other = 1 - c

    w1, w2, w3 = y1p.shape[1] - 2, y2p.shape[1] - 2, y3p.shape[1] - 2

    def parts(*ends):
        return [(first, end - first) for first, end in zip((0,) + ends, ends)]

    z2_ends = (3 * w3 // 4, 5 * w3 // 4, w2)
    y2_ends = [min(end + 1, w2) for end in z2_ends]
    z1_ends = [2 * end for end in y2_ends]
    y1_ends = [min(end + 1, w1) for end in z1_ends]
    z2_parts, y2_parts, z1_parts, y1_parts = parts(*z2_ends), parts(*y2_ends), parts(*z1_ends), parts(*y1_ends)
    x_parts = parts(*[-(-2 * end // images) for end in y1_ends])

    def pair_rows(buf, sections):
        n = buf.shape[0]
        ops = []
        for first, count in sections:
            cells = pl.ds(1 + first // 2, count // 2)
            ops.append(halo(buf.at[n - 1, cells], buf.at[0, cells], down, c, has_down, has_up))
        return ops

    def pair_diag(buf):
        n, w = buf.shape[0], buf.shape[1] - 1
        return halo(buf.at[n - 1, w, 1], buf.at[0, 0, 1], down, other, down_left, up_right)

    def pair_col(buf, first, count):
        w = buf.shape[1] - 1
        return halo(buf.at[pl.ds(first, count), w, 1], buf.at[pl.ds(first, count), 0, 1], r, other, is_left, is_right)

    def plain_down(buf, k0=0, k=None):
        n, w, k = buf.shape[0], buf.shape[1], k or buf.shape[3]
        at = (pl.ds(1, w - 2), pl.ds(0, images), pl.ds(k0, k))
        return halo(buf.at[(n - 2,) + at], buf.at[(0,) + at], down, c, has_down, has_up)

    def plain_ups(buf, sections, k0=0, k=None):
        n, k = buf.shape[0], k or buf.shape[3]
        ops = []
        for first, count in sections:
            at = (pl.ds(1 + first, count), pl.ds(0, images), pl.ds(k0, k))
            ops.append(halo(buf.at[(1,) + at], buf.at[(n - 1,) + at], up, c, has_up, has_down))
        return ops

    def plain_edge(buf):
        w = buf.shape[1]
        return (w - 2) - (w - 3) * c, (w - 1) * c

    def plain_diag(buf, towards_down, k0=0, k=None):
        n, k = buf.shape[0], k or buf.shape[3]
        src_col, dst_col = plain_edge(buf)
        at = (pl.ds(0, images), pl.ds(k0, k))
        if towards_down:
            return halo(buf.at[(n - 2, src_col) + at], buf.at[(0, dst_col) + at], down, other, has_down, has_up)
        return halo(buf.at[(1, src_col) + at], buf.at[(n - 1, dst_col) + at], up, other, has_up, has_down)

    def plain_col(buf, first, count, k0=0, k=None):
        k = k or buf.shape[3]
        src_col, dst_col = plain_edge(buf)
        at = (pl.ds(0, images), pl.ds(k0, k))
        return halo(buf.at[(pl.ds(first, count), src_col) + at], buf.at[(pl.ds(first, count), dst_col) + at], r, other, None, None)

    x_rows = [halo(x_ref.at[:, 7, pl.ds(first, count)], raw_halo.at[:, pl.ds(first, count)], down, c, has_down, has_up) for first, count in x_parts]
    x_diag = pair_diag(xp)
    x_col_b, x_col_a = pair_col(xp, 6, 3), pair_col(xp, 1, 5)
    y1_down, y1_ups = plain_down(y1p), plain_ups(y1p, y1_parts)
    y1_ddown, y1_dup = plain_diag(y1p, True), plain_diag(y1p, False)
    y1_col_b, y1_col_a = plain_col(y1p, 2, 3), plain_col(y1p, 1, 1)
    z1_rows, z1_diag = pair_rows(z1p, z1_parts), pair_diag(z1p)
    z1_cols = [pair_col(z1p, a, n) for a, n in ((1, 1), (2, 2), (4, 1))]
    y2_down, y2_ups = plain_down(y2p), plain_ups(y2p, y2_parts)
    y2_ddown, y2_dup = plain_diag(y2p, True), plain_diag(y2p, False)
    y2_col_b, y2_col_a = plain_col(y2p, 2, 1), plain_col(y2p, 1, 1)
    z2_rows, z2_diag = pair_rows(z2p, z2_parts), pair_diag(z2p)
    z2_cols = [pair_col(z2p, a, 1) for a in (1, 2)]
    y3_halves = []
    for k0 in (0, c2):
        y3_halves.append((plain_col(y3p, 1, 1, k0, c2), plain_diag(y3p, True, k0, c2), plain_diag(y3p, False, k0, c2),
                          plain_down(y3p, k0, c2), plain_ups(y3p, ((0, w3),), k0, c2)[0]))

    assert len(copies) == send_sem.shape[0]

    def under_conditions(items):
        groups = {}
        for condition, action in items:
            groups.setdefault(id(condition), (condition, []))[1].append(action)
        for condition, actions in groups.values():
            def run(actions=actions):
                for action in actions:
                    action()
            if condition is None:
                run()
            else:
                pl.when(condition)(run)

    def start(*ops):
        under_conditions([(send_if, copy.start) for copy, send_if, _ in ops])

    def arrive(*ops):
        under_conditions([(recv_if, copy.wait_recv) for copy, _, recv_if in ops])

    def start_part(rows, diag, i):
        items = [(has_up, rows[i][0].start)]
        if i == 0:
            items.append((up_right, diag[0].start))
        if i == len(rows) - 1:
            items.append((up_left, diag[0].start))
        under_conditions(items)

    def arrive_part(rows, diag, i):
        items = [(has_down, rows[i][0].wait_recv)]
        if i == 0:
            items.append((down_right, diag[0].wait_recv))
        if i == len(rows) - 1:
            items.append((down_left, diag[0].wait_recv))
        under_conditions(items)

    pair_bufs, plain_bufs = (xp, z1p, z2p), (y1p, y2p, y3p)

    @pl.when(has_up == False)
    def _():
        raw_halo[...] = jnp.zeros(raw_halo.shape, BF16)
        for buf in pair_bufs + plain_bufs:
            buf[0] = jnp.zeros(buf.shape[1:], BF16)

    @pl.when(has_down == False)
    def _():
        for buf in plain_bufs:
            buf[buf.shape[0] - 1] = jnp.zeros(buf.shape[1:], BF16)

    @pl.when(is_left)
    def _():
        for buf in pair_bufs:
            buf[:, 0, 1] = jnp.zeros((buf.shape[0],) + buf.shape[3:], BF16)
        for buf in plain_bufs:
            buf[:, 0] = jnp.zeros((buf.shape[0],) + buf.shape[2:], BF16)

    @pl.when(is_right)
    def _():
        for buf in plain_bufs:
            buf[:, buf.shape[1] - 1] = jnp.zeros((buf.shape[0],) + buf.shape[2:], BF16)

    def raw_copy(h):
        slot = h % RAW
        return pltpu.make_async_copy(x_ref.at[:, h], raw.at[slot], raw_sem.at[slot])

    for h in range(7, 7 - RAW, -1):
        raw_copy(h).start()
    for copy in loads_d1:
        copy.start()
    barrier = pltpu.get_barrier_semaphore()

    def signal(row, col):
        pl.semaphore_signal(barrier, inc=1, device_id={"row": row, "col": col}, device_id_type=pl.DeviceIdType.MESH)

    signal(r, other)

    @pl.when(has_up)
    def _():
        signal(up, c)
        signal(up, other)

    @pl.when(has_down)
    def _():
        signal(down, c)
        signal(down, other)

    inner = has_up & has_down

    @pl.when(inner)
    def _():
        pl.semaphore_wait(barrier, 5)

    @pl.when(inner == False)
    def _():
        pl.semaphore_wait(barrier, 3)

    start(*x_rows)

    size = images * images

    def turn(src, index, row, b):
        value = jnp.dot(perm[...], src[index + (slice(None), b)].reshape(size, c0), preferred_element_type=F32)
        xp[row, pl.ds(1 + b * (images // 2), images // 2)] = value.astype(BF16).reshape(images // 2, 2, images, c0)

    blocks = 2 * w1 // images

    def turn_rows(first, count):
        for h in range(first, first - count, -1):
            raw_copy(h).wait()
            for b in range(blocks):
                turn(raw, (h % RAW,), h + 1, b)
            if h >= RAW:
                raw_copy(h - RAW).start()

    def piece(taps, n_all, w, section, slot=None, fresh=True, bias=None, store=None):
        first, count = section
        for n0 in range(0, n_all, part):
            total = None
            for lhs, weight in taps:
                prod = jnp.dot(lhs(first, count), weight(n0), preferred_element_type=F32)
                total = prod if total is None else total + prod
            at = pl.ds((n0 // part) * w * images + first * images, count * images)
            if not fresh:
                total = total + acc[slot, at]
            if store is None:
                acc[slot, at] = total
            else:
                store(n0, jnp.maximum(total + bias[:, pl.ds(n0, part)], 0.0).astype(BF16), first, count)

    def pair_lhs(buf, row, kx):
        return lambda first, count: buf[row, pl.ds(first + (kx + 1) // 2, count), (kx + 1) % 2].reshape(count * images, buf.shape[4])

    def plain_lhs(buf, row, kx, k0=0, k=None):
        k = k or buf.shape[3]
        return lambda first, count: buf[row, pl.ds(first + kx, count), :, pl.ds(k0, k)].reshape(count * images, k)

    def plain_store(buf, h):
        def store(n0, value, first, count):
            buf[h + 1, pl.ds(1 + first, count), :, pl.ds(n0, part)] = value.reshape(count, images, part)
        return store

    def pair_store(buf, h):
        def store(n0, value, first, count):
            buf[h + 1, pl.ds(1 + first // 2, count // 2), :, :, pl.ds(n0, part)] = value.reshape(count // 2, 2, images, part)
        return store

    def down1(h, kys, section=(0, w1), final=True, **kw):
        taps = [(pair_lhs(xp, 2 * h + ky, kx), lambda n0, t=3 * ky + kx: block(place_d1(t), c0, n0)) for ky in kys for kx in TAPS]
        piece(taps, c1, w1, section, bias=bd1, store=plain_store(y1p, h) if final else None, **kw)

    def conv1(h, kys, section=(0, w1), final=True, proj=False, **kw):
        taps = [(plain_lhs(y1p, h + ky, kx), lambda n0, t=3 * ky + kx: block(place_c1(t), c1, n0)) for ky in kys for kx in TAPS]
        if proj:
            taps.append((pair_lhs(xp, 2 * h + 1, 1), lambda n0: block(place_d1(9), c0, n0)))
        piece(taps, c1, w1, section, bias=bc1, store=pair_store(z1p, h) if final else None, **kw)

    def down2(h, kys, section=(0, w2), final=True, **kw):
        taps = [(pair_lhs(z1p, 2 * h + ky, kx), lambda n0, t=3 * ky + kx: block(place_d2(t), c1, n0)) for ky in kys for kx in TAPS]
        piece(taps, c2, w2, section, bias=bd2, store=plain_store(y2p, h) if final else None, **kw)

    def conv2(h, kys, section=(0, w2), final=True, proj=False, **kw):
        taps = [(plain_lhs(y2p, h + ky, kx, kh * c1, c1), lambda n0, t=3 * ky + kx, kh=kh: block(place_c2(t, kh), c1, n0))
                for ky in kys for kx in TAPS for kh in range(2)]
        if proj:
            taps.append((pair_lhs(z1p, 2 * h + 1, 1), lambda n0: block(place_d2(9), c1, n0)))
        piece(taps, c2, w2, section, bias=bc2, store=pair_store(z2p, h) if final else None, **kw)

    m3 = w3 * images

    def group_dots(left, slot, into, fresh=False, n_range=None):
        for n0 in range(*(n_range or (0, c3)), part):
            at = pl.ds((n0 // part) * m3, m3)
            prod = jnp.dot(left, ring[slot, :, pl.ds(n0, part)], preferred_element_type=F32)
            acc[into, at] = prod if fresh else acc[into, at] + prod

    def z2_left(row, kx):
        return z2p[row, pl.ds((kx + 1) // 2, w3), (kx + 1) % 2].reshape(m3, c2)

    def down3(ky, g0):
        for kx in TAPS:
            slot = (g0 + kx + 8) % RING
            first_groups(g0 + kx).wait()
            group_dots(z2_left(ky, kx), slot, 0, fresh=g0 + kx == 0)
            conv3_first(g0 + kx)

    def conv3(first):
        def body(i, carry):
            slot = lax.rem(i + first + 8, RING)
            group_wait(slot)
            if first == 0:
                ky, kx, k0 = 1, i // 2, pl.multiple_of(lax.rem(i, 2) * c2, c2)
            else:
                ky, kx, k0 = 2 * (i // 3), lax.rem(i, 3), (first // 6 - 1) * c2
            left = y3p[ky, pl.ds(kx, w3), :, pl.ds(k0, c2)].reshape(m3, c2)
            group_dots(left, slot, 1)
            if first == 0:
                later = lax.rem(i + 4, 6)
                conv3_copy(6 * (later // 3) + lax.rem(later, 3), pl.multiple_of((i + 4) // 6 * c2, c2), slot).start()
            elif first == 6:
                @pl.when(i < 2)
                def _():
                    conv3_copy(7 + i, c2, slot).start()
            return carry
        lax.fori_loop(0, 6, body, 0)

    turn_rows(7, 3)
    start(x_col_b, x_diag)
    for copy in loads_c1:
        copy.start()
    turn_rows(4, 2)
    for copy in loads_d1:
        copy.wait()
    arrive(x_col_b)
    down1(3, TAPS)
    start(y1_ddown, y1_down)
    for copy in loads_d2:
        copy.start()
    turn_rows(2, 3)
    start(x_col_a)
    for copy in loads_c2:
        copy.start()
    arrive(x_col_a)
    down1(1, TAPS)
    down1(2, TAPS)
    start(y1_col_b)
    down1(0, TAPS[1:], slot=0, **MID)
    for copy in loads_c1:
        copy.wait()
    arrive(y1_col_b)
    conv1(2, TAPS, **PROJ)
    conv1(1, TAPS[1:], **PROJ, slot=1, **MID)
    conv1(3, TAPS[:2], **PROJ, slot=2, **MID)
    arrive(x_diag)
    for i, section in enumerate(y1_parts):
        arrive(x_rows[i])
        for b in range(x_parts[i][0], sum(x_parts[i])):
            turn(raw_halo, (), 0, b)
        down1(0, TAPS[:1], section, slot=0, **END)
        start_part(y1_ups, y1_dup, i)
    start(y1_col_a)
    arrive(y1_col_a)
    conv1(1, TAPS[:1], slot=1, **END)
    start(z1_cols[1])
    conv1(0, TAPS[1:], **PROJ, slot=0, **MID)
    for copy in loads_d2:
        copy.wait()
    arrive(z1_cols[1])
    down2(1, TAPS[:2], slot=1, **MID)
    for i, section in enumerate(z1_parts):
        arrive_part(y1_ups, y1_dup, i)
        conv1(3, TAPS[2:], section, slot=2, **END)
        start(z1_rows[i])
    start(z1_cols[2], z1_diag)
    arrive(y1_down, y1_ddown)
    conv1(0, TAPS[:1], slot=0, **END)
    start(z1_cols[0])
    for g in range(2):
        first_groups(g).start()

    arrive(z1_cols[2])
    down2(1, TAPS[2:], slot=1, **END)
    start(y2_col_b, y2_ddown, y2_down)
    arrive(z1_cols[0])
    down2(0, TAPS[1:], slot=0, **MID)
    for copy in loads_c2:
        copy.wait()
    arrive(y2_col_b)
    conv2(1, TAPS[1:2], **PROJ, slot=1, **MID)
    conv2(0, TAPS[2:], **PROJ, slot=2, **MID)
    for g in (2, 3):
        first_groups(g).start()
    arrive(z1_diag)
    for i, section in enumerate(y2_parts):
        arrive(z1_rows[i])
        down2(0, TAPS[:1], section, slot=0, **END)
        start_part(y2_ups, y2_dup, i)
    start(y2_col_a)
    first_groups(4).start()
    arrive(y2_col_a)
    conv2(1, TAPS[:1], slot=1, **END, **MID)
    conv2(0, TAPS[1:2], slot=2, **END, **MID)
    first_groups(5).start()
    for i, section in enumerate(z2_parts):
        arrive_part(y2_ups, y2_dup, i)
        conv2(1, TAPS[2:], section, slot=1, **END)
        start(z2_rows[i])
    start(z2_cols[1], z2_diag)
    for g in (6, 7):
        first_groups(g).start()
    arrive(y2_down, y2_ddown)
    conv2(0, TAPS[:1], slot=2, **END)
    start(z2_cols[0])
    for g in (8, 9):
        first_groups(g).start()

    arrive(z2_cols[1])
    down3(2, 0)
    arrive(z2_cols[0])
    down3(1, 3)
    first_groups(6).wait()
    group_dots(z2_left(1, 1), (6 + 8) % RING, 1, fresh=True)
    conv3_first(6)
    arrive(*z2_rows, z2_diag)
    for g in range(7, 10):
        first_groups(g).wait()
    for half in range(2):
        for kx in TAPS:
            group_dots(z2_left(0, kx), (kx + 7 + 8) % RING, 0, n_range=(half * c2, half * c2 + c2))
        for n0 in range(half * c2, half * c2 + c2, part):
            total = acc[0, pl.ds((n0 // part) * m3, m3)] + bd3[:, pl.ds(n0, part)]
            y3p[1, pl.ds(1, w3), :, pl.ds(n0, part)] = jnp.maximum(total, 0.0).astype(BF16).reshape(w3, images, part)
        start(*y3_halves[half])
    for j in range(7, 10):
        conv3_first(j)
    arrive(y3_halves[0][0], y3_halves[1][0])
    conv3(0)
    arrive(*y3_halves[0][1:])
    conv3(6)
    arrive(*y3_halves[1][1:])
    conv3(12)
    for n0 in range(0, c3, part):
        total = acc[1, pl.ds((n0 // part) * m3, m3)] + bc3[:, pl.ds(n0, part)]
        out_v[:, :, pl.ds(n0, part)] = jnp.maximum(total, 0.0).astype(BF16).reshape(w3, images, part)
    put = pltpu.make_async_copy(out_v, out_ref, out_sem.at[0])
    put.start()
    under_conditions(copies)
    put.wait()


def solution(mesh):
    row_count = mesh.shape["row"]
    col_count = mesh.shape["col"]
    tile_spec = P("batch", "row", "col")

    def local_blocks(x_tile, *params):
        images, tile_h, tile_w, c0 = x_tile.shape
        weights, biases = [], []
        for stage in TAPS:
            w_down, b_down, w_conv, b_conv, w_proj = params[5 * stage:5 * stage + 5]
            weights += [w_down.reshape((9,) + w_down.shape[2:]), w_conv.reshape((9,) + w_conv.shape[2:]), w_proj]
            biases += [b_down.reshape(1, -1), b_conv.reshape(1, -1)]
        c1, c2, c3 = (weights[3 * stage].shape[2] for stage in TAPS)
        w1, w2, w3 = tile_w // 2, tile_w // 4, tile_w // 8
        any_spec = pl.BlockSpec(memory_space=pl.ANY)
        vmem_spec = pl.BlockSpec(memory_space=pltpu.VMEM)
        index = np.arange(images * images)
        perm = jnp.asarray(index[:, None] == (index % images * images + index // images)[None, :], BF16)
        copy_count = 45
        out = pl.pallas_call(
            lambda *refs: encoder_kernel(row_count, col_count, *refs),
            out_shape=jax.ShapeDtypeStruct((w3, images, c3), BF16),
            in_specs=[any_spec] * 10 + [vmem_spec] * 7,
            out_specs=any_spec,
            scratch_shapes=[
                pltpu.VMEM((tile_h + 1, w1 + 1, 2, images, c0), BF16),
                pltpu.VMEM((6, w1 + 2, images, c1), BF16),
                pltpu.VMEM((5, w2 + 1, 2, images, c1), BF16),
                pltpu.VMEM((4, w2 + 2, images, c2), BF16),
                pltpu.VMEM((3, w3 + 1, 2, images, c2), BF16),
                pltpu.VMEM((3, w3 + 2, images, c3), BF16),
                pltpu.VMEM((RING, c2, c3), BF16),
                pltpu.VMEM((3, w1 * images, c1), F32),
                pltpu.VMEM((w3, images, c3), BF16),
                pltpu.VMEM((RAW, images, tile_w // images, images, c0), BF16),
                pltpu.VMEM((images, tile_w // images, images, c0), BF16),
                pltpu.SemaphoreType.DMA(TAPS[1:2]),
                pltpu.SemaphoreType.DMA((RAW,)),
                pltpu.SemaphoreType.DMA((19,)),
                pltpu.SemaphoreType.DMA((28,)),
                pltpu.SemaphoreType.DMA((RING,)),
                pltpu.SemaphoreType.DMA((copy_count,)),
                pltpu.SemaphoreType.DMA((copy_count,)),
            ],
            compiler_params=pltpu.CompilerParams(collective_id=0, has_side_effects=True, vmem_limit_bytes=67043328),
            name="encoder",
        )(x_tile.reshape(images, tile_h, tile_w // images, images, c0), *weights, *biases, perm)
        return out.transpose(1, 0, 2).reshape(images, 1, w3, c3)

    return jax.shard_map(local_blocks, mesh=mesh, in_specs=(tile_spec,) + (P(),) * 15, out_specs=tile_spec, check_vma=False)
```

```python
import jax
import jax.numpy as jnp
import numpy as np
from jax import lax
from jax.experimental import pallas as pl
from jax.experimental.pallas import tpu as pltpu
from jax.sharding import PartitionSpec as P

F32 = jnp.float32
BF16 = jnp.bfloat16
RING = 10
RAW = 4
TAPS = (0, 1, 2)
MID = dict(final=False)
END = dict(fresh=False)
PROJ = dict(proj=True)


def encoder_kernel(rows, cols, x_ref, wd1, wc1, wp1, wd2, wc2, wp2, wd3, wc3, wp3, bd1, bc1, bd2, bc2, bd3, bc3, perm, out_ref,
                   xp, y1p, z1p, y2p, z2p, y3p, ring, acc, out_v, raw, raw_halo, out_sem, raw_sem, w1_sem, w2_sem, ring_sem, send_sem, recv_sem):
    r = lax.axis_index("row")
    c = lax.axis_index("col")
    has_up = r > 0
    has_down = r < rows - 1
    images = x_ref.shape[0]
    part = acc.shape[2]
    c0, c1, c2, c3 = x_ref.shape[4], wd1.shape[2], wd2.shape[2], wd3.shape[2]

    def place_c1(t):
        if t == 8:
            return 9, 0, 0
        return 8, (t // 4) * c1, (t % 4) * c1

    def place_d1(t):
        return 9, (t % 4) * c0, (1 + t // 4) * c1

    def place_d2(t):
        q = (t - 3 if t < 9 else 6) if t > 2 else 8 + t
        return q // 4, ((q % 4) // 2) * c1, (q % 2) * c2

    def place_c2(tap, kh):
        q = 2 * ((tap + 6) % 9) + kh
        return 3 + q // 4, ((q % 4) // 2) * c1, (q % 2) * c2

    def load(src, place, size, sem):
        slot, k0, n0 = place
        return pltpu.make_async_copy(src, ring.at[slot, pl.ds(k0, size[0]), pl.ds(n0, size[1])], sem)

    def block(place, k, n0):
        slot, k0, n1 = place
        return ring[slot, pl.ds(k0, k), pl.ds(n1 + n0, part)]

    loads_d1 = [load(wd1.at[t], place_d1(t), (c0, c1), w1_sem.at[t]) for t in range(9)]
    loads_d1.append(load(wp1, place_d1(9), (c0, c1), w1_sem.at[9]))
    loads_c1 = [load(wc1.at[t], place_c1(t), (c1, c1), w1_sem.at[10 + t]) for t in range(9)]
    loads_d2 = [load(wd2.at[t], place_d2(t), (c1, c2), w2_sem.at[t]) for t in range(9)]
    loads_d2.append(load(wp2, place_d2(9), (c1, c2), w2_sem.at[9]))
    loads_c2 = [load(wc2.at[q // 2, pl.ds((q % 2) * c1, c1)], place_c2(q // 2, q % 2), (c1, c2), w2_sem.at[10 + q]) for q in range(18)]

    def first_groups(g):
        if g == 6:
            src = wp3
        else:
            ky = 2 if g < 3 else 1 if g < 6 else 0
            kx = g % 3 if g < 6 else g - 7
            src = wd3.at[3 * ky + kx]
        return pltpu.make_async_copy(src, ring.at[(g + 8) % RING], ring_sem.at[(g + 8) % RING])

    def conv3_copy(tap, k0, slot):
        return pltpu.make_async_copy(wc3.at[tap, pl.ds(k0, c2)], ring.at[slot], ring_sem.at[slot])

    def conv3_first(j):
        if j < 6:
            tap, kh = 3 + j // 2, j % 2
        else:
            tap, kh = 6 * ((j - 6) // 3) + (j - 6) % 3, 0
        conv3_copy(tap, kh * c2, (j + 8) % RING).start()

    def group_wait(slot):
        pltpu.make_async_copy(wc3.at[0, pl.ds(0, c2)], ring.at[slot], ring_sem.at[slot]).wait()

    up, down = jnp.maximum(r - 1, 0), jnp.minimum(r + 1, rows - 1)
    copies = []

    def halo(src, dst, row, col, send_if, recv_if):
        index = len(copies)
        copy = pltpu.make_async_remote_copy(src_ref=src, dst_ref=dst, send_sem=send_sem.at[index], recv_sem=recv_sem.at[index],
                                            device_id={"row": row, "col": col}, device_id_type=pl.DeviceIdType.MESH)
        copies.append((send_if, copy.wait_send))
        return copy, send_if, recv_if

    is_left = c == 0
    is_right = c == 1
    up_left, up_right, down_left, down_right = has_up & is_left, has_up & is_right, has_down & is_left, has_down & is_right
    other = 1 - c

    w1, w2, w3 = y1p.shape[1] - 2, y2p.shape[1] - 2, y3p.shape[1] - 2

    def parts(*ends):
        return [(first, end - first) for first, end in zip((0,) + ends, ends)]

    z2_ends = (3 * w3 // 4, 5 * w3 // 4, w2)
    y2_ends = [min(end + 1, w2) for end in z2_ends]
    z1_ends = [2 * end for end in y2_ends]
    y1_ends = [min(end + 1, w1) for end in z1_ends]
    z2_parts, y2_parts, z1_parts, y1_parts = parts(*z2_ends), parts(*y2_ends), parts(*z1_ends), parts(*y1_ends)
    x_parts = parts(*[-(-2 * end // images) for end in y1_ends])

    def pair_rows(buf, sections):
        n = buf.shape[0]
        ops = []
        for first, count in sections:
            cells = pl.ds(1 + first // 2, count // 2)
            ops.append(halo(buf.at[n - 1, cells], buf.at[0, cells], down, c, has_down, has_up))
        return ops

    def pair_diag(buf):
        n, w = buf.shape[0], buf.shape[1] - 1
        return halo(buf.at[n - 1, w, 1], buf.at[0, 0, 1], down, other, down_left, up_right)

    def pair_col(buf, first, count):
        w = buf.shape[1] - 1
        return halo(buf.at[pl.ds(first, count), w, 1], buf.at[pl.ds(first, count), 0, 1], r, other, is_left, is_right)

    def plain_down(buf, k0=0, k=None):
        n, w, k = buf.shape[0], buf.shape[1], k or buf.shape[3]
        at = (pl.ds(1, w - 2), pl.ds(0, images), pl.ds(k0, k))
        return halo(buf.at[(n - 2,) + at], buf.at[(0,) + at], down, c, has_down, has_up)

    def plain_ups(buf, sections, k0=0, k=None):
        n, k = buf.shape[0], k or buf.shape[3]
        ops = []
        for first, count in sections:
            at = (pl.ds(1 + first, count), pl.ds(0, images), pl.ds(k0, k))
            ops.append(halo(buf.at[(1,) + at], buf.at[(n - 1,) + at], up, c, has_up, has_down))
        return ops

    def plain_edge(buf):
        w = buf.shape[1]
        return (w - 2) - (w - 3) * c, (w - 1) * c

    def plain_diag(buf, towards_down, k0=0, k=None):
        n, k = buf.shape[0], k or buf.shape[3]
        src_col, dst_col = plain_edge(buf)
        at = (pl.ds(0, images), pl.ds(k0, k))
        if towards_down:
            return halo(buf.at[(n - 2, src_col) + at], buf.at[(0, dst_col) + at], down, other, has_down, has_up)
        return halo(buf.at[(1, src_col) + at], buf.at[(n - 1, dst_col) + at], up, other, has_up, has_down)

    def plain_col(buf, first, count, k0=0, k=None):
        k = k or buf.shape[3]
        src_col, dst_col = plain_edge(buf)
        at = (pl.ds(0, images), pl.ds(k0, k))
        return halo(buf.at[(pl.ds(first, count), src_col) + at], buf.at[(pl.ds(first, count), dst_col) + at], r, other, None, None)

    x_rows = [halo(x_ref.at[:, 7, pl.ds(first, count)], raw_halo.at[:, pl.ds(first, count)], down, c, has_down, has_up) for first, count in x_parts]
    x_diag = pair_diag(xp)
    x_col_b, x_col_a = pair_col(xp, 6, 3), pair_col(xp, 1, 5)
    y1_down, y1_ups = plain_down(y1p), plain_ups(y1p, y1_parts)
    y1_ddown, y1_dup = plain_diag(y1p, True), plain_diag(y1p, False)
    y1_col_b, y1_col_a = plain_col(y1p, 2, 3), plain_col(y1p, 1, 1)
    z1_rows, z1_diag = pair_rows(z1p, z1_parts), pair_diag(z1p)
    z1_cols = [pair_col(z1p, a, n) for a, n in ((1, 1), (2, 2), (4, 1))]
    y2_down, y2_ups = plain_down(y2p), plain_ups(y2p, y2_parts)
    y2_ddown, y2_dup = plain_diag(y2p, True), plain_diag(y2p, False)
    y2_col_b, y2_col_a = plain_col(y2p, 2, 1), plain_col(y2p, 1, 1)
    z2_rows, z2_diag = pair_rows(z2p, z2_parts), pair_diag(z2p)
    z2_cols = [pair_col(z2p, a, 1) for a in (1, 2)]
    y3_halves = []
    for k0 in (0, c2):
        y3_halves.append((plain_col(y3p, 1, 1, k0, c2), plain_diag(y3p, True, k0, c2), plain_diag(y3p, False, k0, c2),
                          plain_down(y3p, k0, c2), plain_ups(y3p, ((0, w3),), k0, c2)[0]))

    assert len(copies) == send_sem.shape[0]

    def under_conditions(items):
        groups = {}
        for condition, action in items:
            groups.setdefault(id(condition), (condition, []))[1].append(action)
        for condition, actions in groups.values():
            def run(actions=actions):
                for action in actions:
                    action()
            if condition is None:
                run()
            else:
                pl.when(condition)(run)

    def start(*ops):
        under_conditions([(send_if, copy.start) for copy, send_if, _ in ops])

    def arrive(*ops):
        under_conditions([(recv_if, copy.wait_recv) for copy, _, recv_if in ops])

    def start_part(rows, diag, i):
        items = [(has_up, rows[i][0].start)]
        if i == 0:
            items.append((up_right, diag[0].start))
        if i == len(rows) - 1:
            items.append((up_left, diag[0].start))
        under_conditions(items)

    def arrive_part(rows, diag, i):
        items = [(has_down, rows[i][0].wait_recv)]
        if i == 0:
            items.append((down_right, diag[0].wait_recv))
        if i == len(rows) - 1:
            items.append((down_left, diag[0].wait_recv))
        under_conditions(items)

    pair_bufs, plain_bufs = (xp, z1p, z2p), (y1p, y2p, y3p)

    @pl.when(has_up == False)
    def _():
        raw_halo[...] = jnp.zeros(raw_halo.shape, BF16)
        for buf in pair_bufs + plain_bufs:
            buf[0] = jnp.zeros(buf.shape[1:], BF16)

    @pl.when(has_down == False)
    def _():
        for buf in plain_bufs:
            buf[buf.shape[0] - 1] = jnp.zeros(buf.shape[1:], BF16)

    @pl.when(is_left)
    def _():
        for buf in pair_bufs:
            buf[:, 0, 1] = jnp.zeros((buf.shape[0],) + buf.shape[3:], BF16)
        for buf in plain_bufs:
            buf[:, 0] = jnp.zeros((buf.shape[0],) + buf.shape[2:], BF16)

    @pl.when(is_right)
    def _():
        for buf in plain_bufs:
            buf[:, buf.shape[1] - 1] = jnp.zeros((buf.shape[0],) + buf.shape[2:], BF16)

    def raw_copy(h):
        slot = h % RAW
        return pltpu.make_async_copy(x_ref.at[:, h], raw.at[slot], raw_sem.at[slot])

    for h in range(7, 7 - RAW, -1):
        raw_copy(h).start()
    for copy in loads_d1:
        copy.start()
    barrier = pltpu.get_barrier_semaphore()

    def signal(row, col):
        pl.semaphore_signal(barrier, inc=1, device_id={"row": row, "col": col}, device_id_type=pl.DeviceIdType.MESH)

    signal(r, other)

    @pl.when(has_up)
    def _():
        signal(up, c)
        signal(up, other)

    @pl.when(has_down)
    def _():
        signal(down, c)
        signal(down, other)

    inner = has_up & has_down

    @pl.when(inner)
    def _():
        pl.semaphore_wait(barrier, 5)

    @pl.when(inner == False)
    def _():
        pl.semaphore_wait(barrier, 3)

    start(*x_rows)

    size = images * images

    def turn(src, index, row, b):
        value = jnp.dot(perm[...], src[index + (slice(None), b)].reshape(size, c0), preferred_element_type=F32)
        xp[row, pl.ds(1 + b * (images // 2), images // 2)] = value.astype(BF16).reshape(images // 2, 2, images, c0)

    blocks = 2 * w1 // images

    def turn_rows(first, count):
        for h in range(first, first - count, -1):
            raw_copy(h).wait()
            for b in range(blocks):
                turn(raw, (h % RAW,), h + 1, b)
            if h >= RAW:
                raw_copy(h - RAW).start()

    def piece(taps, n_all, w, section, slot=None, fresh=True, bias=None, store=None):
        first, count = section
        for n0 in range(0, n_all, part):
            total = None
            for lhs, weight in taps:
                prod = jnp.dot(lhs(first, count), weight(n0), preferred_element_type=F32)
                total = prod if total is None else total + prod
            at = pl.ds((n0 // part) * w * images + first * images, count * images)
            if not fresh:
                total = total + acc[slot, at]
            if store is None:
                acc[slot, at] = total
            else:
                store(n0, jnp.maximum(total + bias[:, pl.ds(n0, part)], 0.0).astype(BF16), first, count)

    def pair_lhs(buf, row, kx):
        return lambda first, count: buf[row, pl.ds(first + (kx + 1) // 2, count), (kx + 1) % 2].reshape(count * images, buf.shape[4])

    def plain_lhs(buf, row, kx, k0=0, k=None):
        k = k or buf.shape[3]
        return lambda first, count: buf[row, pl.ds(first + kx, count), :, pl.ds(k0, k)].reshape(count * images, k)

    def plain_store(buf, h):
        def store(n0, value, first, count):
            buf[h + 1, pl.ds(1 + first, count), :, pl.ds(n0, part)] = value.reshape(count, images, part)
        return store

    def pair_store(buf, h):
        def store(n0, value, first, count):
            buf[h + 1, pl.ds(1 + first // 2, count // 2), :, :, pl.ds(n0, part)] = value.reshape(count // 2, 2, images, part)
        return store

    def down1(h, kys, section=(0, w1), final=True, **kw):
        taps = [(pair_lhs(xp, 2 * h + ky, kx), lambda n0, t=3 * ky + kx: block(place_d1(t), c0, n0)) for ky in kys for kx in TAPS]
        piece(taps, c1, w1, section, bias=bd1, store=plain_store(y1p, h) if final else None, **kw)

    def conv1(h, kys, section=(0, w1), final=True, proj=False, **kw):
        taps = [(plain_lhs(y1p, h + ky, kx), lambda n0, t=3 * ky + kx: block(place_c1(t), c1, n0)) for ky in kys for kx in TAPS]
        if proj:
            taps.append((pair_lhs(xp, 2 * h + 1, 1), lambda n0: block(place_d1(9), c0, n0)))
        piece(taps, c1, w1, section, bias=bc1, store=pair_store(z1p, h) if final else None, **kw)

    def down2(h, kys, section=(0, w2), final=True, **kw):
        taps = [(pair_lhs(z1p, 2 * h + ky, kx), lambda n0, t=3 * ky + kx: block(place_d2(t), c1, n0)) for ky in kys for kx in TAPS]
        piece(taps, c2, w2, section, bias=bd2, store=plain_store(y2p, h) if final else None, **kw)

    def conv2(h, kys, section=(0, w2), final=True, proj=False, **kw):
        taps = [(plain_lhs(y2p, h + ky, kx, kh * c1, c1), lambda n0, t=3 * ky + kx, kh=kh: block(place_c2(t, kh), c1, n0))
                for ky in kys for kx in TAPS for kh in range(2)]
        if proj:
            taps.append((pair_lhs(z1p, 2 * h + 1, 1), lambda n0: block(place_d2(9), c1, n0)))
        piece(taps, c2, w2, section, bias=bc2, store=pair_store(z2p, h) if final else None, **kw)

    m3 = w3 * images

    def group_dots(left, slot, into, fresh=False, n_range=None):
        for n0 in range(*(n_range or (0, c3)), part):
            at = pl.ds((n0 // part) * m3, m3)
            prod = jnp.dot(left, ring[slot, :, pl.ds(n0, part)], preferred_element_type=F32)
            acc[into, at] = prod if fresh else acc[into, at] + prod

    def z2_left(row, kx):
        return z2p[row, pl.ds((kx + 1) // 2, w3), (kx + 1) % 2].reshape(m3, c2)

    def down3(ky, g0):
        for kx in TAPS:
            slot = (g0 + kx + 8) % RING
            first_groups(g0 + kx).wait()
            group_dots(z2_left(ky, kx), slot, 0, fresh=g0 + kx == 0)
            conv3_first(g0 + kx)

    def conv3(first):
        def body(i, carry):
            slot = lax.rem(i + first + 8, RING)
            group_wait(slot)
            if first == 0:
                ky, kx, k0 = 1, i // 2, pl.multiple_of(lax.rem(i, 2) * c2, c2)
            else:
                ky, kx, k0 = 2 * (i // 3), lax.rem(i, 3), (first // 6 - 1) * c2
            left = y3p[ky, pl.ds(kx, w3), :, pl.ds(k0, c2)].reshape(m3, c2)
            group_dots(left, slot, 1)
            if first == 0:
                later = lax.rem(i + 4, 6)
                conv3_copy(6 * (later // 3) + lax.rem(later, 3), pl.multiple_of((i + 4) // 6 * c2, c2), slot).start()
            elif first == 6:
                @pl.when(i < 2)
                def _():
                    conv3_copy(7 + i, c2, slot).start()
            return carry
        lax.fori_loop(0, 6, body, 0)

    turn_rows(7, 3)
    start(x_col_b, x_diag)
    for copy in loads_c1:
        copy.start()
    turn_rows(4, 2)
    for copy in loads_d1:
        copy.wait()
    arrive(x_col_b)
    down1(3, TAPS)
    start(y1_ddown, y1_down)
    for copy in loads_d2:
        copy.start()
    turn_rows(2, 3)
    start(x_col_a)
    for copy in loads_c2:
        copy.start()
    arrive(x_col_a)
    down1(1, TAPS)
    down1(2, TAPS)
    start(y1_col_b)
    down1(0, TAPS[1:], slot=0, **MID)
    for copy in loads_c1:
        copy.wait()
    arrive(y1_col_b)
    conv1(2, TAPS, **PROJ)
    conv1(1, TAPS[1:], **PROJ, slot=1, **MID)
    conv1(3, TAPS[:2], **PROJ, slot=2, **MID)
    arrive(x_diag)
    for i, section in enumerate(y1_parts):
        arrive(x_rows[i])
        for b in range(x_parts[i][0], sum(x_parts[i])):
            turn(raw_halo, (), 0, b)
        down1(0, TAPS[:1], section, slot=0, **END)
        start_part(y1_ups, y1_dup, i)
    start(y1_col_a)
    arrive(y1_col_a)
    conv1(1, TAPS[:1], slot=1, **END)
    start(z1_cols[1])
    conv1(0, TAPS[1:], **PROJ, slot=0, **MID)
    for copy in loads_d2:
        copy.wait()
    arrive(z1_cols[1])
    down2(1, TAPS[:2], slot=1, **MID)
    for i, section in enumerate(z1_parts):
        arrive_part(y1_ups, y1_dup, i)
        conv1(3, TAPS[2:], section, slot=2, **END)
        start(z1_rows[i])
    start(z1_cols[2], z1_diag)
    arrive(y1_down, y1_ddown)
    conv1(0, TAPS[:1], slot=0, **END)
    start(z1_cols[0])
    for g in range(2):
        first_groups(g).start()

    arrive(z1_cols[2])
    down2(1, TAPS[2:], slot=1, **END)
    start(y2_col_b, y2_ddown, y2_down)
    arrive(z1_cols[0])
    down2(0, TAPS[1:], slot=0, **MID)
    for copy in loads_c2:
        copy.wait()
    arrive(y2_col_b)
    conv2(1, TAPS[1:2], **PROJ, slot=1, **MID)
    conv2(0, TAPS[2:], **PROJ, slot=2, **MID)
    for g in (2, 3):
        first_groups(g).start()
    arrive(z1_diag)
    for i, section in enumerate(y2_parts):
        arrive(z1_rows[i])
        down2(0, TAPS[:1], section, slot=0, **END)
        start_part(y2_ups, y2_dup, i)
    start(y2_col_a)
    first_groups(4).start()
    arrive(y2_col_a)
    conv2(1, TAPS[:1], slot=1, **END, **MID)
    conv2(0, TAPS[1:2], slot=2, **END, **MID)
    first_groups(5).start()
    for i, section in enumerate(z2_parts):
        arrive_part(y2_ups, y2_dup, i)
        conv2(1, TAPS[2:], section, slot=1, **END)
        start(z2_rows[i])
    start(z2_cols[1], z2_diag)
    for g in (6, 7):
        first_groups(g).start()
    arrive(z2_cols[1])
    down3(2, 0)
    arrive(y2_down, y2_ddown)
    conv2(0, TAPS[:1], slot=2, **END)
    start(z2_cols[0])
    for g in (8, 9):
        first_groups(g).start()

    arrive(z2_cols[0])
    down3(1, 3)
    first_groups(6).wait()
    group_dots(z2_left(1, 1), (6 + 8) % RING, 1, fresh=True)
    conv3_first(6)
    arrive(*z2_rows, z2_diag)
    for g in range(7, 10):
        first_groups(g).wait()
    for half in range(2):
        for kx in TAPS:
            group_dots(z2_left(0, kx), (kx + 7 + 8) % RING, 0, n_range=(half * c2, half * c2 + c2))
        for n0 in range(half * c2, half * c2 + c2, part):
            total = acc[0, pl.ds((n0 // part) * m3, m3)] + bd3[:, pl.ds(n0, part)]
            y3p[1, pl.ds(1, w3), :, pl.ds(n0, part)] = jnp.maximum(total, 0.0).astype(BF16).reshape(w3, images, part)
        start(*y3_halves[half])
    for j in range(7, 10):
        conv3_first(j)
    arrive(y3_halves[0][0], y3_halves[1][0])
    conv3(0)
    arrive(*y3_halves[0][1:])
    conv3(6)
    arrive(*y3_halves[1][1:])
    conv3(12)
    for n0 in range(0, c3, part):
        total = acc[1, pl.ds((n0 // part) * m3, m3)] + bc3[:, pl.ds(n0, part)]
        out_v[:, :, pl.ds(n0, part)] = jnp.maximum(total, 0.0).astype(BF16).reshape(w3, images, part)
    put = pltpu.make_async_copy(out_v, out_ref, out_sem.at[0])
    put.start()
    under_conditions(copies)
    put.wait()


def solution(mesh):
    row_count = mesh.shape["row"]
    col_count = mesh.shape["col"]
    tile_spec = P("batch", "row", "col")

    def local_blocks(x_tile, *params):
        images, tile_h, tile_w, c0 = x_tile.shape
        weights, biases = [], []
        for stage in TAPS:
            w_down, b_down, w_conv, b_conv, w_proj = params[5 * stage:5 * stage + 5]
            weights += [w_down.reshape((9,) + w_down.shape[2:]), w_conv.reshape((9,) + w_conv.shape[2:]), w_proj]
            biases += [b_down.reshape(1, -1), b_conv.reshape(1, -1)]
        c1, c2, c3 = (weights[3 * stage].shape[2] for stage in TAPS)
        w1, w2, w3 = tile_w // 2, tile_w // 4, tile_w // 8
        any_spec = pl.BlockSpec(memory_space=pl.ANY)
        vmem_spec = pl.BlockSpec(memory_space=pltpu.VMEM)
        index = np.arange(images * images)
        perm = jnp.asarray(index[:, None] == (index % images * images + index // images)[None, :], BF16)
        copy_count = 45
        out = pl.pallas_call(
            lambda *refs: encoder_kernel(row_count, col_count, *refs),
            out_shape=jax.ShapeDtypeStruct((w3, images, c3), BF16),
            in_specs=[any_spec] * 10 + [vmem_spec] * 7,
            out_specs=any_spec,
            scratch_shapes=[
                pltpu.VMEM((tile_h + 1, w1 + 1, 2, images, c0), BF16),
                pltpu.VMEM((6, w1 + 2, images, c1), BF16),
                pltpu.VMEM((5, w2 + 1, 2, images, c1), BF16),
                pltpu.VMEM((4, w2 + 2, images, c2), BF16),
                pltpu.VMEM((3, w3 + 1, 2, images, c2), BF16),
                pltpu.VMEM((3, w3 + 2, images, c3), BF16),
                pltpu.VMEM((RING, c2, c3), BF16),
                pltpu.VMEM((3, w1 * images, c1), F32),
                pltpu.VMEM((w3, images, c3), BF16),
                pltpu.VMEM((RAW, images, tile_w // images, images, c0), BF16),
                pltpu.VMEM((images, tile_w // images, images, c0), BF16),
                pltpu.SemaphoreType.DMA(TAPS[1:2]),
                pltpu.SemaphoreType.DMA((RAW,)),
                pltpu.SemaphoreType.DMA((19,)),
                pltpu.SemaphoreType.DMA((28,)),
                pltpu.SemaphoreType.DMA((RING,)),
                pltpu.SemaphoreType.DMA((copy_count,)),
                pltpu.SemaphoreType.DMA((copy_count,)),
            ],
            compiler_params=pltpu.CompilerParams(collective_id=0, has_side_effects=True, vmem_limit_bytes=67043328),
            name="encoder",
        )(x_tile.reshape(images, tile_h, tile_w // images, images, c0), *weights, *biases, perm)
        return out.transpose(1, 0, 2).reshape(images, 1, w3, c3)

    return jax.shard_map(local_blocks, mesh=mesh, in_specs=(tile_spec,) + (P(),) * 15, out_specs=tile_spec, check_vma=False)
```

```python
import jax
import jax.numpy as jnp
import numpy as np
from jax import lax
from jax.experimental import pallas as pl
from jax.experimental.pallas import tpu as pltpu
from jax.sharding import PartitionSpec as P

F32 = jnp.float32
BF16 = jnp.bfloat16
RING = 10
RAW = 4
TAPS = (0, 1, 2)
MID = dict(final=False)
END = dict(fresh=False)
PROJ = dict(proj=True)


def encoder_kernel(rows, cols, x_ref, wd1, wc1, wp1, wd2, wc2, wp2, wd3, wc3, wp3, bd1, bc1, bd2, bc2, bd3, bc3, perm, out_ref,
                   xp, y1p, z1p, y2p, z2p, y3p, ring, acc, out_v, raw, raw_halo, out_sem, raw_sem, w1_sem, w2_sem, ring_sem, send_sem, recv_sem):
    r = lax.axis_index("row")
    c = lax.axis_index("col")
    has_up = r > 0
    has_down = r < rows - 1
    images = x_ref.shape[0]
    part = acc.shape[2]
    c0, c1, c2, c3 = x_ref.shape[4], wd1.shape[2], wd2.shape[2], wd3.shape[2]

    def place_c1(t):
        if t == 8:
            return 9, 0, 0
        return 8, (t // 4) * c1, (t % 4) * c1

    def place_d1(t):
        return 9, (t % 4) * c0, (1 + t // 4) * c1

    def place_d2(t):
        q = (t - 3 if t < 9 else 6) if t > 2 else 8 + t
        return q // 4, ((q % 4) // 2) * c1, (q % 2) * c2

    def place_c2(tap, kh):
        q = 2 * ((tap + 6) % 9) + kh
        return 3 + q // 4, ((q % 4) // 2) * c1, (q % 2) * c2

    def load(src, place, size, sem):
        slot, k0, n0 = place
        return pltpu.make_async_copy(src, ring.at[slot, pl.ds(k0, size[0]), pl.ds(n0, size[1])], sem)

    def block(place, k, n0):
        slot, k0, n1 = place
        return ring[slot, pl.ds(k0, k), pl.ds(n1 + n0, part)]

    loads_d1 = [load(wd1.at[t], place_d1(t), (c0, c1), w1_sem.at[t]) for t in range(9)]
    loads_d1.append(load(wp1, place_d1(9), (c0, c1), w1_sem.at[9]))
    loads_c1 = [load(wc1.at[t], place_c1(t), (c1, c1), w1_sem.at[10 + t]) for t in range(9)]
    loads_d2 = [load(wd2.at[t], place_d2(t), (c1, c2), w2_sem.at[t]) for t in range(9)]
    loads_d2.append(load(wp2, place_d2(9), (c1, c2), w2_sem.at[9]))
    loads_c2 = [load(wc2.at[q // 2, pl.ds((q % 2) * c1, c1)], place_c2(q // 2, q % 2), (c1, c2), w2_sem.at[10 + q]) for q in range(18)]

    def first_groups(g):
        if g == 6:
            src = wp3
        else:
            ky = 2 if g < 3 else 1 if g < 6 else 0
            kx = g % 3 if g < 6 else g - 7
            src = wd3.at[3 * ky + kx]
        return pltpu.make_async_copy(src, ring.at[(g + 8) % RING], ring_sem.at[(g + 8) % RING])

    def conv3_copy(tap, k0, slot):
        return pltpu.make_async_copy(wc3.at[tap, pl.ds(k0, c2)], ring.at[slot], ring_sem.at[slot])

    def conv3_first(j):
        if j < 6:
            tap, kh = 3 + j // 2, j % 2
        else:
            tap, kh = 6 * ((j - 6) // 3) + (j - 6) % 3, 0
        conv3_copy(tap, kh * c2, (j + 8) % RING).start()

    def group_wait(slot):
        pltpu.make_async_copy(wc3.at[0, pl.ds(0, c2)], ring.at[slot], ring_sem.at[slot]).wait()

    up, down = jnp.maximum(r - 1, 0), jnp.minimum(r + 1, rows - 1)
    copies = []

    def halo(src, dst, row, col, send_if, recv_if):
        index = len(copies)
        copy = pltpu.make_async_remote_copy(src_ref=src, dst_ref=dst, send_sem=send_sem.at[index], recv_sem=recv_sem.at[index],
                                            device_id={"row": row, "col": col}, device_id_type=pl.DeviceIdType.MESH)
        copies.append((send_if, copy.wait_send))
        return copy, send_if, recv_if

    is_left = c == 0
    is_right = c == 1
    up_left, up_right, down_left, down_right = has_up & is_left, has_up & is_right, has_down & is_left, has_down & is_right
    other = 1 - c

    w1, w2, w3 = y1p.shape[1] - 2, y2p.shape[1] - 2, y3p.shape[1] - 2

    def parts(*ends):
        return [(first, end - first) for first, end in zip((0,) + ends, ends)]

    z2_ends = (3 * w3 // 4, 5 * w3 // 4, w2)
    y2_ends = [min(end + 1, w2) for end in z2_ends]
    z1_ends = [2 * end for end in y2_ends]
    y1_ends = [min(end + 1, w1) for end in z1_ends]
    z2_parts, y2_parts, z1_parts, y1_parts = parts(*z2_ends), parts(*y2_ends), parts(*z1_ends), parts(*y1_ends)
    x_parts = parts(*[-(-2 * end // images) for end in y1_ends])

    def pair_rows(buf, sections):
        n = buf.shape[0]
        ops = []
        for first, count in sections:
            cells = pl.ds(1 + first // 2, count // 2)
            ops.append(halo(buf.at[n - 1, cells], buf.at[0, cells], down, c, has_down, has_up))
        return ops

    def pair_diag(buf):
        n, w = buf.shape[0], buf.shape[1] - 1
        return halo(buf.at[n - 1, w, 1], buf.at[0, 0, 1], down, other, down_left, up_right)

    def pair_col(buf, first, count):
        w = buf.shape[1] - 1
        return halo(buf.at[pl.ds(first, count), w, 1], buf.at[pl.ds(first, count), 0, 1], r, other, is_left, is_right)

    def plain_down(buf, k0=0, k=None):
        n, w, k = buf.shape[0], buf.shape[1], k or buf.shape[3]
        at = (pl.ds(1, w - 2), pl.ds(0, images), pl.ds(k0, k))
        return halo(buf.at[(n - 2,) + at], buf.at[(0,) + at], down, c, has_down, has_up)

    def plain_ups(buf, sections, k0=0, k=None):
        n, k = buf.shape[0], k or buf.shape[3]
        ops = []
        for first, count in sections:
            at = (pl.ds(1 + first, count), pl.ds(0, images), pl.ds(k0, k))
            ops.append(halo(buf.at[(1,) + at], buf.at[(n - 1,) + at], up, c, has_up, has_down))
        return ops

    def plain_edge(buf):
        w = buf.shape[1]
        return (w - 2) - (w - 3) * c, (w - 1) * c

    def plain_diag(buf, towards_down, k0=0, k=None):
        n, k = buf.shape[0], k or buf.shape[3]
        src_col, dst_col = plain_edge(buf)
        at = (pl.ds(0, images), pl.ds(k0, k))
        if towards_down:
            return halo(buf.at[(n - 2, src_col) + at], buf.at[(0, dst_col) + at], down, other, has_down, has_up)
        return halo(buf.at[(1, src_col) + at], buf.at[(n - 1, dst_col) + at], up, other, has_up, has_down)

    def plain_col(buf, first, count, k0=0, k=None):
        k = k or buf.shape[3]
        src_col, dst_col = plain_edge(buf)
        at = (pl.ds(0, images), pl.ds(k0, k))
        return halo(buf.at[(pl.ds(first, count), src_col) + at], buf.at[(pl.ds(first, count), dst_col) + at], r, other, None, None)

    x_rows = [halo(x_ref.at[:, 7, pl.ds(first, count)], raw_halo.at[:, pl.ds(first, count)], down, c, has_down, has_up) for first, count in x_parts]
    x_diag = pair_diag(xp)
    x_col_b, x_col_a = pair_col(xp, 6, 3), pair_col(xp, 1, 5)
    y1_down, y1_ups = plain_down(y1p), plain_ups(y1p, y1_parts)
    y1_ddown, y1_dup = plain_diag(y1p, True), plain_diag(y1p, False)
    y1_col_b, y1_col_a = plain_col(y1p, 2, 3), plain_col(y1p, 1, 1)
    z1_rows, z1_diag = pair_rows(z1p, z1_parts), pair_diag(z1p)
    z1_cols = [pair_col(z1p, a, n) for a, n in ((1, 1), (2, 2), (4, 1))]
    y2_down, y2_ups = plain_down(y2p), plain_ups(y2p, y2_parts)
    y2_ddown, y2_dup = plain_diag(y2p, True), plain_diag(y2p, False)
    y2_col_b, y2_col_a = plain_col(y2p, 2, 1), plain_col(y2p, 1, 1)
    z2_rows, z2_diag = pair_rows(z2p, z2_parts), pair_diag(z2p)
    z2_cols = [pair_col(z2p, a, 1) for a in (1, 2)]
    y3_halves = []
    for k0 in (0, c2):
        y3_halves.append((plain_col(y3p, 1, 1, k0, c2), plain_diag(y3p, True, k0, c2), plain_diag(y3p, False, k0, c2),
                          plain_down(y3p, k0, c2), plain_ups(y3p, ((0, w3),), k0, c2)[0]))

    assert len(copies) == send_sem.shape[0]

    def under_conditions(items):
        groups = {}
        for condition, action in items:
            groups.setdefault(id(condition), (condition, []))[1].append(action)
        for condition, actions in groups.values():
            def run(actions=actions):
                for action in actions:
                    action()
            if condition is None:
                run()
            else:
                pl.when(condition)(run)

    def start(*ops):
        under_conditions([(send_if, copy.start) for copy, send_if, _ in ops])

    def arrive(*ops):
        under_conditions([(recv_if, copy.wait_recv) for copy, _, recv_if in ops])

    def start_part(rows, diag, i):
        items = [(has_up, rows[i][0].start)]
        if i == 0:
            items.append((up_right, diag[0].start))
        if i == len(rows) - 1:
            items.append((up_left, diag[0].start))
        under_conditions(items)

    def arrive_part(rows, diag, i):
        items = [(has_down, rows[i][0].wait_recv)]
        if i == 0:
            items.append((down_right, diag[0].wait_recv))
        if i == len(rows) - 1:
            items.append((down_left, diag[0].wait_recv))
        under_conditions(items)

    pair_bufs, plain_bufs = (xp, z1p, z2p), (y1p, y2p, y3p)

    @pl.when(has_up == False)
    def _():
        raw_halo[...] = jnp.zeros(raw_halo.shape, BF16)
        for buf in pair_bufs + plain_bufs:
            buf[0] = jnp.zeros(buf.shape[1:], BF16)

    @pl.when(has_down == False)
    def _():
        for buf in plain_bufs:
            buf[buf.shape[0] - 1] = jnp.zeros(buf.shape[1:], BF16)

    @pl.when(is_left)
    def _():
        for buf in pair_bufs:
            buf[:, 0, 1] = jnp.zeros((buf.shape[0],) + buf.shape[3:], BF16)
        for buf in plain_bufs:
            buf[:, 0] = jnp.zeros((buf.shape[0],) + buf.shape[2:], BF16)

    @pl.when(is_right)
    def _():
        for buf in plain_bufs:
            buf[:, buf.shape[1] - 1] = jnp.zeros((buf.shape[0],) + buf.shape[2:], BF16)

    def raw_copy(h):
        slot = h % RAW
        return pltpu.make_async_copy(x_ref.at[:, h], raw.at[slot], raw_sem.at[slot])

    for h in range(7, 7 - RAW, -1):
        raw_copy(h).start()
    for copy in loads_d1:
        copy.start()
    barrier = pltpu.get_barrier_semaphore()

    def signal(row, col):
        pl.semaphore_signal(barrier, inc=1, device_id={"row": row, "col": col}, device_id_type=pl.DeviceIdType.MESH)

    signal(r, other)

    @pl.when(has_up)
    def _():
        signal(up, c)
        signal(up, other)

    @pl.when(has_down)
    def _():
        signal(down, c)
        signal(down, other)

    inner = has_up & has_down

    @pl.when(inner)
    def _():
        pl.semaphore_wait(barrier, 5)

    @pl.when(inner == False)
    def _():
        pl.semaphore_wait(barrier, 3)

    start(*x_rows)

    size = images * images

    def turn(src, index, row, b):
        value = jnp.dot(perm[...], src[index + (slice(None), b)].reshape(size, c0), preferred_element_type=F32)
        xp[row, pl.ds(1 + b * (images // 2), images // 2)] = value.astype(BF16).reshape(images // 2, 2, images, c0)

    blocks = 2 * w1 // images

    def turn_rows(first, count):
        for h in range(first, first - count, -1):
            raw_copy(h).wait()
            for b in range(blocks):
                turn(raw, (h % RAW,), h + 1, b)
            if h >= RAW:
                raw_copy(h - RAW).start()

    def piece(taps, n_all, w, section, slot=None, fresh=True, bias=None, store=None):
        first, count = section
        for n0 in range(0, n_all, part):
            total = None
            for lhs, weight in taps:
                prod = jnp.dot(lhs(first, count), weight(n0), preferred_element_type=F32)
                total = prod if total is None else total + prod
            at = pl.ds((n0 // part) * w * images + first * images, count * images)
            if not fresh:
                total = total + acc[slot, at]
            if store is None:
                acc[slot, at] = total
            else:
                store(n0, jnp.maximum(total + bias[:, pl.ds(n0, part)], 0.0).astype(BF16), first, count)

    def pair_lhs(buf, row, kx):
        return lambda first, count: buf[row, pl.ds(first + (kx + 1) // 2, count), (kx + 1) % 2].reshape(count * images, buf.shape[4])

    def plain_lhs(buf, row, kx, k0=0, k=None):
        k = k or buf.shape[3]
        return lambda first, count: buf[row, pl.ds(first + kx, count), :, pl.ds(k0, k)].reshape(count * images, k)

    def plain_store(buf, h):
        def store(n0, value, first, count):
            buf[h + 1, pl.ds(1 + first, count), :, pl.ds(n0, part)] = value.reshape(count, images, part)
        return store

    def pair_store(buf, h):
        def store(n0, value, first, count):
            buf[h + 1, pl.ds(1 + first // 2, count // 2), :, :, pl.ds(n0, part)] = value.reshape(count // 2, 2, images, part)
        return store

    def down1(h, kys, section=(0, w1), final=True, **kw):
        taps = [(pair_lhs(xp, 2 * h + ky, kx), lambda n0, t=3 * ky + kx: block(place_d1(t), c0, n0)) for ky in kys for kx in TAPS]
        piece(taps, c1, w1, section, bias=bd1, store=plain_store(y1p, h) if final else None, **kw)

    def conv1(h, kys, section=(0, w1), final=True, proj=False, **kw):
        taps = [(plain_lhs(y1p, h + ky, kx), lambda n0, t=3 * ky + kx: block(place_c1(t), c1, n0)) for ky in kys for kx in TAPS]
        if proj:
            taps.append((pair_lhs(xp, 2 * h + 1, 1), lambda n0: block(place_d1(9), c0, n0)))
        piece(taps, c1, w1, section, bias=bc1, store=pair_store(z1p, h) if final else None, **kw)

    def down2(h, kys, section=(0, w2), final=True, **kw):
        taps = [(pair_lhs(z1p, 2 * h + ky, kx), lambda n0, t=3 * ky + kx: block(place_d2(t), c1, n0)) for ky in kys for kx in TAPS]
        piece(taps, c2, w2, section, bias=bd2, store=plain_store(y2p, h) if final else None, **kw)

    def conv2(h, kys, section=(0, w2), final=True, proj=False, **kw):
        taps = [(plain_lhs(y2p, h + ky, kx, kh * c1, c1), lambda n0, t=3 * ky + kx, kh=kh: block(place_c2(t, kh), c1, n0))
                for ky in kys for kx in TAPS for kh in range(2)]
        if proj:
            taps.append((pair_lhs(z1p, 2 * h + 1, 1), lambda n0: block(place_d2(9), c1, n0)))
        piece(taps, c2, w2, section, bias=bc2, store=pair_store(z2p, h) if final else None, **kw)

    m3 = w3 * images

    def group_dots(left, slot, into, fresh=False, n_range=None):
        for n0 in range(*(n_range or (0, c3)), part):
            at = pl.ds((n0 // part) * m3, m3)
            prod = jnp.dot(left, ring[slot, :, pl.ds(n0, part)], preferred_element_type=F32)
            acc[into, at] = prod if fresh else acc[into, at] + prod

    def z2_left(row, kx):
        return z2p[row, pl.ds((kx + 1) // 2, w3), (kx + 1) % 2].reshape(m3, c2)

    def down3(ky, g0):
        for kx in TAPS:
            slot = (g0 + kx + 8) % RING
            first_groups(g0 + kx).wait()
            group_dots(z2_left(ky, kx), slot, 0, fresh=g0 + kx == 0)
            conv3_first(g0 + kx)

    def conv3(first):
        def body(i, carry):
            slot = lax.rem(i + first + 8, RING)
            group_wait(slot)
            if first == 0:
                ky, kx, k0 = 1, i // 2, pl.multiple_of(lax.rem(i, 2) * c2, c2)
            else:
                ky, kx, k0 = 2 * (i // 3), lax.rem(i, 3), (first // 6 - 1) * c2
            left = y3p[ky, pl.ds(kx, w3), :, pl.ds(k0, c2)].reshape(m3, c2)
            group_dots(left, slot, 1)
            if first == 0:
                later = lax.rem(i + 4, 6)
                conv3_copy(6 * (later // 3) + lax.rem(later, 3), pl.multiple_of((i + 4) // 6 * c2, c2), slot).start()
            elif first == 6:
                @pl.when(i < 2)
                def _():
                    conv3_copy(7 + i, c2, slot).start()
            return carry
        lax.fori_loop(0, 6, body, 0)

    turn_rows(7, 3)
    start(x_col_b, x_diag)
    for copy in loads_c1:
        copy.start()
    turn_rows(4, 2)
    for copy in loads_d1:
        copy.wait()
    arrive(x_col_b)
    down1(3, TAPS)
    start(y1_ddown, y1_down)
    for copy in loads_d2:
        copy.start()
    turn_rows(2, 3)
    start(x_col_a)
    for copy in loads_c2:
        copy.start()
    arrive(x_col_a)
    down1(1, TAPS)
    down1(2, TAPS)
    start(y1_col_b)
    down1(0, TAPS[1:], slot=0, **MID)
    for copy in loads_c1:
        copy.wait()
    arrive(y1_col_b)
    arrive(x_diag)
    fill = (lambda: conv1(2, TAPS, **PROJ), lambda: conv1(1, TAPS[1:], **PROJ, slot=1, **MID), lambda: conv1(3, TAPS[:2], **PROJ, slot=2, **MID))
    for i, section in enumerate(y1_parts):
        fill[i]()
        arrive(x_rows[i])
        for b in range(x_parts[i][0], sum(x_parts[i])):
            turn(raw_halo, (), 0, b)
        down1(0, TAPS[:1], section, slot=0, **END)
        start_part(y1_ups, y1_dup, i)
    start(y1_col_a)
    arrive(y1_col_a)
    conv1(1, TAPS[:1], slot=1, **END)
    start(z1_cols[1])
    conv1(0, TAPS[1:], **PROJ, slot=0, **MID)
    for copy in loads_d2:
        copy.wait()
    arrive(z1_cols[1])
    down2(1, TAPS[:2], slot=1, **MID)
    for i, section in enumerate(z1_parts):
        arrive_part(y1_ups, y1_dup, i)
        conv1(3, TAPS[2:], section, slot=2, **END)
        start(z1_rows[i])
    start(z1_cols[2], z1_diag)
    arrive(y1_down, y1_ddown)
    conv1(0, TAPS[:1], slot=0, **END)
    start(z1_cols[0])
    for g in range(2):
        first_groups(g).start()

    arrive(z1_cols[2])
    down2(1, TAPS[2:], slot=1, **END)
    start(y2_col_b, y2_ddown, y2_down)
    arrive(z1_cols[0])
    down2(0, TAPS[1:], slot=0, **MID)
    for copy in loads_c2:
        copy.wait()
    arrive(y2_col_b)
    conv2(1, TAPS[1:2], **PROJ, slot=1, **MID)
    conv2(0, TAPS[2:], **PROJ, slot=2, **MID)
    for g in (2, 3):
        first_groups(g).start()
    arrive(z1_diag)
    for i, section in enumerate(y2_parts):
        arrive(z1_rows[i])
        down2(0, TAPS[:1], section, slot=0, **END)
        start_part(y2_ups, y2_dup, i)
    start(y2_col_a)
    first_groups(4).start()
    arrive(y2_col_a)
    conv2(1, TAPS[:1], slot=1, **END, **MID)
    conv2(0, TAPS[1:2], slot=2, **END, **MID)
    first_groups(5).start()
    for i, section in enumerate(z2_parts):
        arrive_part(y2_ups, y2_dup, i)
        conv2(1, TAPS[2:], section, slot=1, **END)
        start(z2_rows[i])
    start(z2_cols[1], z2_diag)
    for g in (6, 7):
        first_groups(g).start()
    arrive(z2_cols[1])
    down3(2, 0)
    arrive(y2_down, y2_ddown)
    conv2(0, TAPS[:1], slot=2, **END)
    start(z2_cols[0])
    for g in (8, 9):
        first_groups(g).start()

    arrive(z2_cols[0])
    down3(1, 3)
    first_groups(6).wait()
    group_dots(z2_left(1, 1), (6 + 8) % RING, 1, fresh=True)
    conv3_first(6)
    arrive(*z2_rows, z2_diag)
    for g in range(7, 10):
        first_groups(g).wait()
    for half in range(2):
        for kx in TAPS:
            group_dots(z2_left(0, kx), (kx + 7 + 8) % RING, 0, n_range=(half * c2, half * c2 + c2))
        for n0 in range(half * c2, half * c2 + c2, part):
            total = acc[0, pl.ds((n0 // part) * m3, m3)] + bd3[:, pl.ds(n0, part)]
            y3p[1, pl.ds(1, w3), :, pl.ds(n0, part)] = jnp.maximum(total, 0.0).astype(BF16).reshape(w3, images, part)
        start(*y3_halves[half])
    for j in range(7, 10):
        conv3_first(j)
    arrive(y3_halves[0][0], y3_halves[1][0])
    conv3(0)
    arrive(*y3_halves[0][1:])
    conv3(6)
    arrive(*y3_halves[1][1:])
    conv3(12)
    for n0 in range(0, c3, part):
        total = acc[1, pl.ds((n0 // part) * m3, m3)] + bc3[:, pl.ds(n0, part)]
        out_v[:, :, pl.ds(n0, part)] = jnp.maximum(total, 0.0).astype(BF16).reshape(w3, images, part)
    put = pltpu.make_async_copy(out_v, out_ref, out_sem.at[0])
    put.start()
    under_conditions(copies)
    put.wait()


def solution(mesh):
    row_count = mesh.shape["row"]
    col_count = mesh.shape["col"]
    tile_spec = P("batch", "row", "col")

    def local_blocks(x_tile, *params):
        images, tile_h, tile_w, c0 = x_tile.shape
        weights, biases = [], []
        for stage in TAPS:
            w_down, b_down, w_conv, b_conv, w_proj = params[5 * stage:5 * stage + 5]
            weights += [w_down.reshape((9,) + w_down.shape[2:]), w_conv.reshape((9,) + w_conv.shape[2:]), w_proj]
            biases += [b_down.reshape(1, -1), b_conv.reshape(1, -1)]
        c1, c2, c3 = (weights[3 * stage].shape[2] for stage in TAPS)
        w1, w2, w3 = tile_w // 2, tile_w // 4, tile_w // 8
        any_spec = pl.BlockSpec(memory_space=pl.ANY)
        vmem_spec = pl.BlockSpec(memory_space=pltpu.VMEM)
        index = np.arange(images * images)
        perm = jnp.asarray(index[:, None] == (index % images * images + index // images)[None, :], BF16)
        copy_count = 45
        out = pl.pallas_call(
            lambda *refs: encoder_kernel(row_count, col_count, *refs),
            out_shape=jax.ShapeDtypeStruct((w3, images, c3), BF16),
            in_specs=[any_spec] * 10 + [vmem_spec] * 7,
            out_specs=any_spec,
            scratch_shapes=[
                pltpu.VMEM((tile_h + 1, w1 + 1, 2, images, c0), BF16),
                pltpu.VMEM((6, w1 + 2, images, c1), BF16),
                pltpu.VMEM((5, w2 + 1, 2, images, c1), BF16),
                pltpu.VMEM((4, w2 + 2, images, c2), BF16),
                pltpu.VMEM((3, w3 + 1, 2, images, c2), BF16),
                pltpu.VMEM((3, w3 + 2, images, c3), BF16),
                pltpu.VMEM((RING, c2, c3), BF16),
                pltpu.VMEM((3, w1 * images, c1), F32),
                pltpu.VMEM((w3, images, c3), BF16),
                pltpu.VMEM((RAW, images, tile_w // images, images, c0), BF16),
                pltpu.VMEM((images, tile_w // images, images, c0), BF16),
                pltpu.SemaphoreType.DMA(TAPS[1:2]),
                pltpu.SemaphoreType.DMA((RAW,)),
                pltpu.SemaphoreType.DMA((19,)),
                pltpu.SemaphoreType.DMA((28,)),
                pltpu.SemaphoreType.DMA((RING,)),
                pltpu.SemaphoreType.DMA((copy_count,)),
                pltpu.SemaphoreType.DMA((copy_count,)),
            ],
            compiler_params=pltpu.CompilerParams(collective_id=0, has_side_effects=True, vmem_limit_bytes=67043328),
            name="encoder",
        )(x_tile.reshape(images, tile_h, tile_w // images, images, c0), *weights, *biases, perm)
        return out.transpose(1, 0, 2).reshape(images, 1, w3, c3)

    return jax.shard_map(local_blocks, mesh=mesh, in_specs=(tile_spec,) + (P(),) * 15, out_specs=tile_spec, check_vma=False)
```
